8 devices in a mesh: sweep: 1 (over z), data: 2 (over y), ent: 4 (over x, core).
Axes of the slice: x: 2, y: 2, z: 1, core: 2. Of those that a mesh axis runs over, the one named last changes fastest.
Arguments:
- ent_table: float32 [65536, 400], P(('sweep', 'ent'))
- ada_state: float32 [65536], P(('sweep', 'ent'))
- rel_table: float32 [14824, 400], P('sweep')
- head_idx: int32 [4, 2, 4, 8192], P(('sweep', 'ent'), 'data')
- tail_idx: int32 [4, 2, 4, 8192], P(('sweep', 'ent'), 'data')
- rel_idx: int32 [4, 2, 4, 8192], P(('sweep', 'ent'), 'data')
- edge_mask: int32 [4, 2, 4, 8192], P(('sweep', 'ent'), 'data')
- neg_idx: int32 [4, 2, 4, 200], P(('sweep', 'ent'), 'data')
Outputs:
- output 1: float32 [65536, 400], P(('sweep', 'ent'))
- output 2: float32 [65536], P(('sweep', 'ent'))
- output 3: float32 [14824, 400], P('sweep')
- output 4: float32 [4, 2, 4], P(('sweep', 'ent'), 'data')
All inputs are finite; a program needn't handle non-finite values.
Results may differ from the reference program's by a relative error of at most 0.001.
Values are sent between devices in bfloat16 or wider.
A program may use at most 1 GiB of HBM per device.

```python
import jax
import jax.numpy as jnp
from jax import lax

ENT_PARTS = 4
DATA_SHARDS = 2
ENT_ROWS = 16384
DIM = 400
RELS = 14824
NEGS = 200
EDGES = 8192

TOTAL_ROWS = ENT_PARTS * ENT_ROWS
HOT_ROWS = max(ENT_ROWS // 16, 1)
HOT_RELS = max(RELS // 16, 1)
LEARN_ENT = 0.1
LEARN_REL = 0.05
ADA_EPS = 1e-6


def mixed_index(key, idx_shape, full_span, hot_span):
    key_coin, key_hot, key_all = jax.random.split(key, 3)
    coin_flip = jax.random.randint(key_coin, idx_shape, 0, 2)
    hot_pick = jax.random.randint(key_hot, idx_shape, 0, hot_span)
    any_pick = jax.random.randint(key_all, idx_shape, 0, full_span)
    return jnp.where(coin_flip == 1, hot_pick, any_pick).astype(jnp.int32)


def setup_inputs(seed: int = 0, part: int = 0) -> dict:
    base_key = jax.random.fold_in(jax.random.key(seed), part)
    key_list = jax.random.split(base_key, 9)
    ent_scale = (2.0 * DIM) ** -0.25
    edge_shape = (ENT_PARTS, DATA_SHARDS, ENT_PARTS, EDGES)
    fill_level = jax.random.randint(key_list[6], (ENT_PARTS, DATA_SHARDS, ENT_PARTS, 1), 1, 17)
    return {
        "ent_table": jax.random.normal(key_list[0], (TOTAL_ROWS, DIM), jnp.float32) * ent_scale,
        "ada_state": jax.random.uniform(key_list[1], (TOTAL_ROWS,), jnp.float32, 0.5, 2.0) * (ent_scale * ent_scale),
        "rel_table": jax.random.normal(key_list[2], (RELS, DIM), jnp.float32),
        "head_idx": mixed_index(key_list[3], edge_shape, ENT_ROWS, HOT_ROWS),
        "tail_idx": mixed_index(key_list[4], edge_shape, ENT_ROWS, HOT_ROWS),
        "rel_idx": mixed_index(key_list[5], edge_shape, RELS, HOT_RELS),
        "edge_mask": (jax.random.randint(key_list[7], edge_shape, 0, 16) < fill_level).astype(jnp.int32),
        "neg_idx": mixed_index(key_list[8], (ENT_PARTS, DATA_SHARDS, ENT_PARTS, NEGS), ENT_ROWS, HOT_ROWS),
    }


def complex_mul(left, right):
    half_dim = left.shape[-1] // 2
    left_re, left_im = left[..., :half_dim], left[..., half_dim:]
    right_re, right_im = right[..., :half_dim], right[..., half_dim:]
    return jnp.concatenate([left_re * right_re - left_im * right_im, left_re * right_im + left_im * right_re], axis=-1)


def complex_mul_conj(left, right):
    half_dim = left.shape[-1] // 2
    left_re, left_im = left[..., :half_dim], left[..., half_dim:]
    right_re, right_im = right[..., :half_dim], right[..., half_dim:]
    return jnp.concatenate([left_re * right_re + left_im * right_im, left_im * right_re - left_re * right_im], axis=-1)


def bucket_grads(head_rows, tail_rows, neg_rows, rel_rows, weight):
    query_vec = complex_mul(head_rows, rel_rows)
    tail_f32 = tail_rows.astype(jnp.float32)
    pos_score = jnp.sum(query_vec * tail_f32, axis=-1)
    query_bf = query_vec.astype(jnp.bfloat16)
    neg_score = jnp.dot(query_bf, neg_rows.T, preferred_element_type=jnp.float32)
    top_score = jnp.maximum(pos_score, jnp.max(neg_score, axis=-1))
    pos_exp = jnp.exp(pos_score - top_score)
    neg_exp = jnp.exp(neg_score - top_score[:, None])
    norm_sum = pos_exp + jnp.sum(neg_exp, axis=-1)
    loss_sum = jnp.sum(weight * (top_score + jnp.log(norm_sum) - pos_score))
    pos_coef = weight * (pos_exp / norm_sum - 1.0)
    neg_coef = ((weight / norm_sum)[:, None] * neg_exp).astype(jnp.bfloat16)
    query_grad = pos_coef[:, None] * tail_f32 + jnp.dot(neg_coef, neg_rows, preferred_element_type=jnp.float32)
    tail_grad = pos_coef[:, None] * query_vec
    neg_grad = jnp.dot(neg_coef.T, query_bf, preferred_element_type=jnp.float32)
    head_grad = complex_mul_conj(query_grad, rel_rows)
    rel_grad = complex_mul_conj(query_grad, head_rows)
    return head_grad, tail_grad, neg_grad, rel_grad, loss_sum


def reference(ent_table, ada_state, rel_table, head_idx, tail_idx, rel_idx, edge_mask, neg_idx):
    bucket_count = ENT_PARTS * DATA_SHARDS
    head_part = jnp.repeat(jnp.arange(ENT_PARTS, dtype=jnp.int32), DATA_SHARDS)[:, None]

    def one_round(round_carry, round_idx):
        ent_cur, state_cur, rel_cur, rel_state = round_carry
        tail_part = (head_part + round_idx) % ENT_PARTS
        head_ids = head_idx[:, :, round_idx].reshape(bucket_count, EDGES) + head_part * ENT_ROWS
        tail_ids = tail_idx[:, :, round_idx].reshape(bucket_count, EDGES) + tail_part * ENT_ROWS
        neg_ids = neg_idx[:, :, round_idx].reshape(bucket_count, NEGS) + tail_part * ENT_ROWS
        rel_ids = rel_idx[:, :, round_idx].reshape(bucket_count, EDGES)
        weights = edge_mask[:, :, round_idx].reshape(bucket_count, EDGES).astype(jnp.float32)
        table_bf = ent_cur.astype(jnp.bfloat16)

        def one_bucket(acc_carry, bucket):
            row_acc, rel_acc = acc_carry
            bucket_head, bucket_tail, bucket_neg, bucket_rel, bucket_weight = bucket
            head_grad, tail_grad, neg_grad, rel_grad, loss_sum = bucket_grads(
                ent_cur[bucket_head], table_bf[bucket_tail], table_bf[bucket_neg], rel_cur[bucket_rel], bucket_weight)
            row_ids = jnp.concatenate([bucket_head, bucket_tail, bucket_neg])
            row_acc = row_acc.at[row_ids].add(jnp.concatenate([head_grad, tail_grad, neg_grad], axis=0))
            rel_acc = rel_acc.at[bucket_rel].add(rel_grad)
            return (row_acc, rel_acc), loss_sum

        acc_init = (jnp.zeros((TOTAL_ROWS, DIM), jnp.float32), jnp.zeros((RELS, DIM), jnp.float32))
        grad_pair, loss_sums = lax.scan(one_bucket, acc_init, (head_ids, tail_ids, neg_ids, rel_ids, weights))
        row_grad, rel_grad = grad_pair
        state_cur = state_cur + jnp.mean(row_grad * row_grad, axis=-1)
        ent_cur = ent_cur - LEARN_ENT * row_grad / jnp.sqrt(state_cur + ADA_EPS)[:, None]
        rel_state = rel_state + jnp.mean(rel_grad * rel_grad, axis=-1)
        rel_cur = rel_cur - LEARN_REL * rel_grad / jnp.sqrt(rel_state + ADA_EPS)[:, None]
        return (ent_cur, state_cur, rel_cur, rel_state), loss_sums.reshape(ENT_PARTS, DATA_SHARDS) / EDGES

    carry_init = (ent_table, ada_state, rel_table, jnp.zeros((RELS,), jnp.float32))
    carry_end, round_loss = lax.scan(one_round, carry_init, jnp.arange(ENT_PARTS, dtype=jnp.int32))
    return (carry_end[0], carry_end[1], carry_end[2], jnp.transpose(round_loss, (1, 2, 0)))
```

```python
import functools

import jax
import jax.numpy as jnp
from jax import lax
from jax.experimental import pallas as pl
from jax.experimental.pallas import tpu as pltpu
from jax.sharding import PartitionSpec as P

LEARN_ENT = 0.1
LEARN_REL = 0.05
ADA_EPS = 1e-6
LANES = 128
BLOCK = 256
VMEM_CAP = 66_000_000


def pair_at(row):
    return pl.ds(pl.multiple_of(row, 2), 2)


def halves(ref):
    count = ref.shape[0] // 2
    return ref[pl.ds(0, count, stride=2), :], ref[pl.ds(1, count, stride=2), :]


def put_halves(ref, real, imag):
    count = ref.shape[0] // 2
    ref[pl.ds(0, count, stride=2), :] = real
    ref[pl.ds(1, count, stride=2), :] = imag


def query_kernel(head_ref, rel_ref, ent_hbm, rel_hbm, a_ref, r_ref, q_ref, ent_v, rel_v, sems):
    @pl.when(pl.program_id(0) == 0)
    def _():
        first = pltpu.make_async_copy(ent_hbm, ent_v, sems.at[0])
        second = pltpu.make_async_copy(rel_hbm, rel_v, sems.at[1])
        first.start()
        second.start()
        first.wait()
        second.wait()

    unroll = 32

    def some(step, carry):
        for sub in range(unroll):
            edge = step * unroll + sub
            a_ref[pair_at(2 * edge), :] = ent_v[pair_at(head_ref[0, 0, edge]), :]
            r_ref[pair_at(2 * edge), :] = rel_v[pair_at(rel_ref[0, 0, edge]), :]
        return carry

    lax.fori_loop(0, BLOCK // unroll, some, 0)
    a_re, a_im = halves(a_ref)
    r_re, r_im = halves(r_ref)
    q_ref[:, :LANES] = (a_re * r_re - a_im * r_im).astype(jnp.bfloat16)
    q_ref[:, LANES:] = (a_re * r_im + a_im * r_re).astype(jnp.bfloat16)


def tail_kernel(tail_ref, a_ref, r_ref, tab_hbm, c_ref, p_ref, tab_bf, tab_v, sem):
    @pl.when(pl.program_id(0) == 0)
    def _():
        copy = pltpu.make_async_copy(tab_hbm, tab_bf, sem)
        copy.start()
        copy.wait()
        rows = 512

        def widen(step, carry):
            at = pl.ds(pl.multiple_of(step * rows, rows), rows)
            tab_v[at, :] = tab_bf[at, :].astype(jnp.float32)
            return carry

        lax.fori_loop(0, tab_v.shape[0] // rows, widen, 0)

    unroll = 32

    def some(step, carry):
        for sub in range(unroll):
            edge = step * unroll + sub
            c_ref[pair_at(2 * edge), :] = tab_v[pair_at(tail_ref[0, 0, edge]), :]
        return carry

    lax.fori_loop(0, BLOCK // unroll, some, 0)
    a_re, a_im = halves(a_ref)
    r_re, r_im = halves(r_ref)
    c_re, c_im = halves(c_ref)
    prod = (a_re * r_re - a_im * r_im) * c_re + (a_re * r_im + a_im * r_re) * c_im
    p_ref[0] = jnp.sum(prod.T, axis=0, keepdims=True)


def column(row):
    return jnp.broadcast_to(row, (LANES, row.shape[-1])).T


def grad_kernel(
    per_bucket, negs,
    head_ref, tail_ref, rel_ref, neg_ref, a_ref, r_ref, c_ref, qp_ref, pm_ref, pp_ref, w_ref, mm_ref, mp_ref,
    gh_hbm, gt_hbm, gr_hbm, loss_ref,
    acc_h, acc_t, acc_r, blk_h, blk_t, blk_r, neg_acc, sems,
):
    block = pl.program_id(0)
    in_bucket = lax.rem(block, per_bucket)

    @pl.when(block == 0)
    def _():
        for acc in (acc_h, acc_t, acc_r):
            rows = 16

            def clear(step, carry):
                acc[pl.ds(pl.multiple_of(step * rows, rows), rows), :] = jnp.zeros((rows, LANES), jnp.float32)
                return carry

            lax.fori_loop(0, acc.shape[0] // rows, clear, 0)

    @pl.when(in_bucket == 0)
    def _():
        neg_acc[...] = jnp.zeros_like(neg_acc)
        loss_ref[...] = jnp.zeros_like(loss_ref)

    a_re, a_im = halves(a_ref)
    r_re, r_im = halves(r_ref)
    c_re, c_im = halves(c_ref)
    q_re = a_re * r_re - a_im * r_im
    q_im = a_re * r_im + a_im * r_re
    q_bf = jnp.concatenate([q_re.astype(jnp.bfloat16), q_im.astype(jnp.bfloat16)], axis=1)
    m_mine = mm_ref[0]
    nt = (((1,), (1,)), ((), ()))
    score = lax.dot_general(q_bf, m_mine, nt, preferred_element_type=jnp.float32)
    score = score + lax.dot_general(qp_ref[...], mp_ref[0], nt, preferred_element_type=jnp.float32)
    lane = lax.broadcasted_iota(jnp.int32, score.shape, 1)
    score = jnp.where(lane < negs, score, -jnp.inf)
    pos = column(pm_ref[0] + pp_ref[0])
    weight = column(w_ref[0])
    low, high = score[:, :LANES], score[:, LANES:]
    top = jnp.maximum(pos, jnp.max(jnp.maximum(low, high), axis=1, keepdims=True))
    pos_exp = jnp.exp(pos - top)
    low_exp, high_exp = jnp.exp(low - top), jnp.exp(high - top)
    norm = pos_exp + jnp.sum(low_exp + high_exp, axis=1, keepdims=True)
    loss_ref[0] = loss_ref[0] + jnp.sum(weight * (top + jnp.log(norm) - pos), axis=0, keepdims=True)
    alpha = weight * (pos_exp / norm - 1.0)
    scale = weight / norm
    beta = jnp.concatenate([(scale * low_exp).astype(jnp.bfloat16), (scale * high_exp).astype(jnp.bfloat16)], axis=1)
    nn = (((1,), (0,)), ((), ()))
    mixed = lax.dot_general(beta, m_mine, nn, preferred_element_type=jnp.float32)
    tn = (((0,), (0,)), ((), ()))
    neg_acc[...] += lax.dot_general(beta, q_bf, tn, preferred_element_type=jnp.float32)
    d_re = alpha * c_re + mixed[:, :LANES]
    d_im = alpha * c_im + mixed[:, LANES:]
    put_halves(blk_t, alpha * q_re, alpha * q_im)
    put_halves(blk_h, d_re * r_re + d_im * r_im, d_im * r_re - d_re * r_im)
    put_halves(blk_r, d_re * a_re + d_im * a_im, d_im * a_re - d_re * a_im)

    unroll = 16

    def some(step, carry):
        for sub in range(unroll):
            edge = step * unroll + sub
            here = pair_at(2 * edge)
            at_h, at_t, at_r = (pair_at(ref[0, 0, edge]) for ref in (head_ref, tail_ref, rel_ref))
            acc_h[at_h, :] = acc_h[at_h, :] + blk_h[here, :]
            acc_t[at_t, :] = acc_t[at_t, :] + blk_t[here, :]
            acc_r[at_r, :] = acc_r[at_r, :] + blk_r[here, :]
        return carry

    lax.fori_loop(0, BLOCK // unroll, some, 0)

    @pl.when(in_bucket == per_bucket - 1)
    def _():
        put_halves(blk_t, neg_acc[:, :LANES], neg_acc[:, LANES:])
        small = 8

        def more(step, carry):
            for sub in range(small):
                row = step * small + sub
                at_t = pair_at(neg_ref[0, 0, row])
                acc_t[at_t, :] = acc_t[at_t, :] + blk_t[pair_at(2 * row), :]
            return carry

        lax.fori_loop(0, negs // small, more, 0)

    @pl.when(block == pl.num_programs(0) - 1)
    def _():
        copies = [
            pltpu.make_async_copy(acc, out, sems.at[slot])
            for slot, (acc, out) in enumerate(((acc_h, gh_hbm), (acc_t, gt_hbm), (acc_r, gr_hbm)))
        ]
        for copy in copies:
            copy.start()
        for copy in copies:
            copy.wait()


def smem_block(width):
    return pl.BlockSpec((1, 1, width), lambda b: (b, 0, 0), memory_space=pltpu.SMEM)


PAIRS = pl.BlockSpec((2 * BLOCK, LANES), lambda b: (b, 0))
WIDE = pl.BlockSpec((BLOCK, 2 * LANES), lambda b: (b, 0))
ROW = pl.BlockSpec((1, 1, BLOCK), lambda b: (b, 0, 0))
ANYWHERE = pl.BlockSpec(memory_space=pl.ANY)
PARAMS = dict(dimension_semantics=("arbitrary",), vmem_limit_bytes=VMEM_CAP)


def query_rows(ent, rel, head_ids, rel_ids):
    blocks = head_ids.shape[0]
    edges = blocks * BLOCK
    return pl.pallas_call(
        query_kernel,
        grid=(blocks,),
        in_specs=[smem_block(BLOCK), smem_block(BLOCK), ANYWHERE, ANYWHERE],
        out_specs=[PAIRS, PAIRS, WIDE],
        out_shape=[
            jax.ShapeDtypeStruct((2 * edges, LANES), jnp.float32),
            jax.ShapeDtypeStruct((2 * edges, LANES), jnp.float32),
            jax.ShapeDtypeStruct((edges, 2 * LANES), jnp.bfloat16),
        ],
        scratch_shapes=[
            pltpu.VMEM(ent.shape, jnp.float32),
            pltpu.VMEM(rel.shape, jnp.float32),
            pltpu.SemaphoreType.DMA((2,)),
        ],
        compiler_params=pltpu.CompilerParams(**PARAMS),
        cost_estimate=pl.CostEstimate(flops=200_000_000, bytes_accessed=80_000_000, transcendentals=0),
        name="query_rows",
    )(head_ids, rel_ids, ent, rel)


def tail_rows(table, tail_ids, a_rows, r_rows):
    blocks = tail_ids.shape[0]
    edges = blocks * BLOCK
    return pl.pallas_call(
        tail_kernel,
        grid=(blocks,),
        in_specs=[smem_block(BLOCK), PAIRS, PAIRS, ANYWHERE],
        out_specs=[PAIRS, ROW],
        out_shape=[
            jax.ShapeDtypeStruct((2 * edges, LANES), jnp.float32),
            jax.ShapeDtypeStruct((blocks, 1, BLOCK), jnp.float32),
        ],
        scratch_shapes=[
            pltpu.VMEM(table.shape, jnp.bfloat16),
            pltpu.VMEM(table.shape, jnp.float32),
            pltpu.SemaphoreType.DMA,
        ],
        compiler_params=pltpu.CompilerParams(**PARAMS),
        cost_estimate=pl.CostEstimate(flops=200_000_000, bytes_accessed=60_000_000, transcendentals=0),
        name="tail_rows",
    )(tail_ids, a_rows, r_rows, table)


def bucket_grads(ids, neg_ids, rows, q_peer, p_mine, p_peer, weight, m_mine, m_peer, ent_shape, rel_shape, negs):
    head_ids, tail_ids, rel_ids = ids
    blocks = head_ids.shape[0]
    buckets = neg_ids.shape[0]
    per_bucket = blocks // buckets
    of_bucket = lambda b: (b // per_bucket, 0, 0)
    neg_block = pl.BlockSpec((1, 2 * LANES, 2 * LANES), of_bucket)
    return pl.pallas_call(
        functools.partial(grad_kernel, per_bucket, negs),
        grid=(blocks,),
        in_specs=[
            smem_block(BLOCK), smem_block(BLOCK), smem_block(BLOCK),
            pl.BlockSpec((1, 1, neg_ids.shape[-1]), of_bucket, memory_space=pltpu.SMEM),
            PAIRS, PAIRS, PAIRS, WIDE, ROW, ROW, ROW, neg_block, neg_block,
        ],
        out_specs=[ANYWHERE, ANYWHERE, ANYWHERE, pl.BlockSpec((1, 1, LANES), of_bucket)],
        out_shape=[
            jax.ShapeDtypeStruct(ent_shape, jnp.float32),
            jax.ShapeDtypeStruct(ent_shape, jnp.float32),
            jax.ShapeDtypeStruct(rel_shape, jnp.float32),
            jax.ShapeDtypeStruct((buckets, 1, LANES), jnp.float32),
        ],
        scratch_shapes=[
            pltpu.VMEM(ent_shape, jnp.float32),
            pltpu.VMEM(ent_shape, jnp.float32),
            pltpu.VMEM(rel_shape, jnp.float32),
            pltpu.VMEM((2 * BLOCK, LANES), jnp.float32),
            pltpu.VMEM((2 * BLOCK, LANES), jnp.float32),
            pltpu.VMEM((2 * BLOCK, LANES), jnp.float32),
            pltpu.VMEM((2 * LANES, 2 * LANES), jnp.float32),
            pltpu.SemaphoreType.DMA((3,)),
        ],
        compiler_params=pltpu.CompilerParams(**PARAMS),
        cost_estimate=pl.CostEstimate(flops=500_000_000, bytes_accessed=110_000_000, transcendentals=4_000_000),
        name="bucket_grads",
    )(head_ids, tail_ids, rel_ids, neg_ids, *rows, q_peer, p_mine, p_peer, weight, m_mine, m_peer)


def split_columns(table, part):
    rows, dim = table.shape
    width = dim // 4
    flipped = table.T.reshape(2, 2, width, rows)
    mine = lax.dynamic_index_in_dim(flipped, part, axis=1, keepdims=False)
    mine = jnp.pad(mine, ((0, 0), (0, LANES - width), (0, 0)))
    return jnp.transpose(mine, (2, 0, 1)).reshape(2 * rows, LANES)


def join_columns(half, dim):
    rows = half.shape[0] // 2
    width = dim // 4
    flipped = jnp.transpose(half.reshape(rows, 2, LANES)[:, :, :width], (1, 2, 0))
    both = lax.all_gather(flipped, "data", axis=1)
    return both.reshape(dim, rows).T


def adagrad(param, state, grad, rate, dim):
    rows = state.shape[0]
    grad3 = grad.reshape(rows, 2, LANES)
    square = lax.psum(jnp.sum(grad3 * grad3, axis=(1, 2)), "data")
    state = state + square / dim
    step = rate * lax.rsqrt(state + ADA_EPS)
    param = param.reshape(rows, 2, LANES) - grad3 * step[:, None, None]
    return param.reshape(2 * rows, LANES), state


def solution(mesh):
    ent_size = mesh.shape["ent"]
    data_size = mesh.shape["data"]
    swap = [(src, data_size - 1 - src) for src in range(data_size)]

    def device_epoch(ent_table, ada_state, rel_table, head_idx, tail_idx, rel_idx, edge_mask, neg_idx):
        dim = ent_table.shape[1]
        edge_count = head_idx.shape[-1]
        negs = neg_idx.shape[-1]
        part = lax.axis_index("data")
        ent = split_columns(ent_table, part)
        rel = split_columns(rel_table, part)
        state = ada_state
        rel_state = jnp.zeros((rel_table.shape[0],), jnp.float32)

        local = jnp.concatenate(
            [2 * head_idx[0, 0], 2 * tail_idx[0, 0], 2 * rel_idx[0, 0], edge_mask[0, 0], 2 * neg_idx[0, 0]], axis=1)
        both = lax.all_gather(local, "data")
        blocks = data_size * edge_count // BLOCK

        def field(slot, round_idx):
            return both[:, round_idx, slot * edge_count:(slot + 1) * edge_count].reshape(blocks, 1, BLOCK)

        losses = []
        for round_idx in range(ent_size):
            head_ids, tail_ids, rel_ids = (field(slot, round_idx) for slot in range(3))
            weight = field(3, round_idx).astype(jnp.float32)
            neg_ids = both[:, round_idx, 4 * edge_count:].reshape(data_size, 1, negs)
            table = ent.astype(jnp.bfloat16)
            if round_idx:
                fetch = [((dest + round_idx) % ent_size, dest) for dest in range(ent_size)]
                table = lax.ppermute(table, "ent", fetch)
            a_rows, r_rows, q_mine = query_rows(ent, rel, head_ids, rel_ids)
            q_peer = lax.ppermute(q_mine, "data", swap)
            c_rows, p_mine = tail_rows(table, tail_ids, a_rows, r_rows)
            m_mine = jnp.take(table.reshape(-1, 2, LANES), neg_ids.reshape(-1) // 2, axis=0)
            m_mine = m_mine.reshape(data_size, negs, 2 * LANES)
            m_mine = jnp.pad(m_mine, ((0, 0), (0, 2 * LANES - negs), (0, 0)))
            m_peer = lax.ppermute(m_mine, "data", swap)
            p_peer = lax.ppermute(p_mine, "data", swap)
            g_head, g_tail, g_rel, loss = bucket_grads(
                (head_ids, tail_ids, rel_ids), neg_ids, (a_rows, r_rows, c_rows), q_peer, p_mine, p_peer, weight,
                m_mine, m_peer, ent.shape, rel.shape, negs)
            if round_idx:
                back = [(src, (src + round_idx) % ent_size) for src in range(ent_size)]
                g_tail = lax.ppermute(g_tail, "ent", back)
            g_rel = lax.psum(g_rel, "ent")
            ent, state = adagrad(ent, state, g_head + g_tail, LEARN_ENT, dim)
            rel, rel_state = adagrad(rel, rel_state, g_rel, LEARN_REL, dim)
            losses.append(lax.dynamic_index_in_dim(loss, part, axis=0, keepdims=False)[0, 0] / edge_count)
        ent_out = join_columns(ent, dim)
        rel_out = join_columns(rel, dim)
        return ent_out, state, rel_out, jnp.stack(losses)[None, None, :]

    ent_spec = P(("sweep", "ent"), None)
    row_spec = P(("sweep", "ent"))
    rel_spec = P("sweep", None)
    edge_spec = P(("sweep", "ent"), "data", None, None)
    loss_spec = P(("sweep", "ent"), "data", None)
    return jax.shard_map(
        device_epoch, mesh=mesh,
        in_specs=(ent_spec, row_spec, rel_spec, edge_spec, edge_spec, edge_spec, edge_spec, edge_spec),
        out_specs=(ent_spec, row_spec, rel_spec, loss_spec),
        check_vma=False)
```

```python
import functools

import jax
import jax.numpy as jnp
from jax import lax
from jax.experimental import pallas as pl
from jax.experimental.pallas import tpu as pltpu
from jax.sharding import PartitionSpec as P


LEARN_ENT = 0.1
LEARN_REL = 0.05
ADA_EPS = 1e-6
LANES = 128
BLOCK = 256
WIDE_ROWS = 512
VMEM_CAP = 66_000_000


def pair_at(row):
    return pl.ds(pl.multiple_of(row, 2), 2)


def halves(ref):
    count = ref.shape[0] // 2
    return ref[pl.ds(0, count, stride=2), :], ref[pl.ds(1, count, stride=2), :]


def put_halves(ref, real, imag):
    count = ref.shape[0] // 2
    ref[pl.ds(0, count, stride=2), :] = real
    ref[pl.ds(1, count, stride=2), :] = imag


def split_kernel(width, part_ref, in_ref, out_ref, *bf_refs):
    second = part_ref[0] != 0
    lane = lax.broadcasted_iota(jnp.int32, (out_ref.shape[0] // 2, LANES), 1)

    def pick(start):
        last = in_ref.shape[0] - LANES
        shift = max(start - last, 0)
        rows = in_ref[pl.ds(start - shift, LANES), :].T
        if shift:
            rows = pltpu.roll(rows, LANES - shift, 1)
        return jnp.where(lane < width, rows, 0.0)

    real = jnp.where(second, pick(width), pick(0))
    imag = jnp.where(second, pick(3 * width), pick(2 * width))
    put_halves(out_ref, real, imag)
    for ref in bf_refs:
        ref[...] = out_ref[...].astype(jnp.bfloat16)


def split_columns(table, part, with_bf):
    rows, dim = table.shape
    pairs = pl.BlockSpec((2 * WIDE_ROWS, LANES), lambda b: (b, 0))
    kinds = [jnp.float32, jnp.bfloat16] if with_bf else [jnp.float32]
    return pl.pallas_call(
        functools.partial(split_kernel, dim // 4),
        grid=(pl.cdiv(rows, WIDE_ROWS),),
        in_specs=[pl.BlockSpec(memory_space=pltpu.SMEM), pl.BlockSpec((dim, WIDE_ROWS), lambda b: (0, b))],
        out_specs=[pairs] * len(kinds),
        out_shape=[jax.ShapeDtypeStruct((2 * rows, LANES), kind) for kind in kinds],
        compiler_params=pltpu.CompilerParams(dimension_semantics=("arbitrary",)),
        cost_estimate=pl.CostEstimate(flops=20_000_000, bytes_accessed=45_000_000, transcendentals=0),
        name="split_columns",
    )(part[None], table.T)


def flip_kernel(in_ref, out_ref):
    real, imag = halves(in_ref)
    width = out_ref.shape[1]
    out_ref[0] = real.T[:width, :]
    out_ref[1] = imag.T[:width, :]


def flip_half(half, dim):
    rows = half.shape[0] // 2
    return pl.pallas_call(
        flip_kernel,
        grid=(pl.cdiv(rows, WIDE_ROWS),),
        in_specs=[pl.BlockSpec((2 * WIDE_ROWS, LANES), lambda b: (b, 0))],
        out_specs=pl.BlockSpec((2, dim // 4, WIDE_ROWS), lambda b: (0, 0, b)),
        out_shape=jax.ShapeDtypeStruct((2, dim // 4, rows), jnp.float32),
        compiler_params=pltpu.CompilerParams(dimension_semantics=("arbitrary",)),
        cost_estimate=pl.CostEstimate(flops=20_000_000, bytes_accessed=30_000_000, transcendentals=0),
        name="flip_half",
    )(half)


def query_kernel(core_ref, head_ref, rel_ref, ent_hbm, relm_hbm, relo_hbm, a_ref, r_ref, q_ref, ent_v, rel_v, sems):
    @pl.when(pl.program_id(0) == 0)
    def _():
        half = relm_hbm.shape[0]
        core = core_ref[0]
        mine = pl.ds(pl.multiple_of(core * half, 8), half)
        other = pl.ds(pl.multiple_of((1 - core) * half, 8), half)
        copies = [
            pltpu.make_async_copy(ent_hbm, ent_v, sems.at[0]),
            pltpu.make_async_copy(relm_hbm, rel_v.at[mine], sems.at[1]),
            pltpu.make_async_copy(relo_hbm, rel_v.at[other], sems.at[2]),
        ]
        for copy in copies:
            copy.start()
        for copy in copies:
            copy.wait()

    unroll = 32

    def some(step, carry):
        for sub in range(unroll):
            edge = step * unroll + sub
            a_ref[pair_at(2 * edge), :] = ent_v[pair_at(head_ref[0, 0, edge]), :]
            r_ref[pair_at(2 * edge), :] = rel_v[pair_at(rel_ref[0, 0, edge]), :]
        return carry

    lax.fori_loop(0, BLOCK // unroll, some, 0)
    a_re, a_im = halves(a_ref)
    r_re, r_im = halves(r_ref)
    q_ref[:, :LANES] = (a_re * r_re - a_im * r_im).astype(jnp.bfloat16)
    q_ref[:, LANES:] = (a_re * r_im + a_im * r_re).astype(jnp.bfloat16)


def tail_kernel(negs, tail_ref, neg_ref, a_ref, r_ref, tab_hbm, c_ref, p_ref, m_ref, tab_bf, tab_v, neg_v, sem):
    @pl.when(pl.program_id(0) == 0)
    def _():
        copy = pltpu.make_async_copy(tab_hbm, tab_bf, sem)
        copy.start()
        copy.wait()
        rows = 512

        def widen(step, carry):
            at = pl.ds(pl.multiple_of(step * rows, rows), rows)
            tab_v[at, :] = tab_bf[at, :].astype(jnp.float32)
            return carry

        lax.fori_loop(0, tab_v.shape[0] // rows, widen, 0)
        neg_v[...] = jnp.zeros_like(neg_v)
        small = 8

        def pick(step, carry):
            for sub in range(small):
                row = step * small + sub
                neg_v[pair_at(2 * row), :] = tab_v[pair_at(neg_ref[0, 0, row]), :]
            return carry

        lax.fori_loop(0, negs // small, pick, 0)
        m_re, m_im = halves(neg_v)
        m_ref[:, :LANES] = m_re.astype(jnp.bfloat16)
        m_ref[:, LANES:] = m_im.astype(jnp.bfloat16)

    unroll = 32

    def some(step, carry):
        for sub in range(unroll):
            edge = step * unroll + sub
            c_ref[pair_at(2 * edge), :] = tab_v[pair_at(tail_ref[0, 0, edge]), :]
        return carry

    lax.fori_loop(0, BLOCK // unroll, some, 0)
    a_re, a_im = halves(a_ref)
    r_re, r_im = halves(r_ref)
    c_re, c_im = halves(c_ref)
    prod = (a_re * r_re - a_im * r_im) * c_re + (a_re * r_im + a_im * r_re) * c_im
    p_ref[0] = jnp.sum(prod.T, axis=0, keepdims=True)


def column(row):
    return jnp.broadcast_to(row, (LANES, row.shape[-1])).T


def grad_kernel(
    last, negs,
    core_ref, head_ref, tail_ref, rel_ref, neg_ref, a_ref, r_ref, c_ref, qm_ref, qp_ref, pm_ref, pp_ref, w_ref, mm_ref, mp_ref,
    *rest,
):
    before, rest = rest[:3 * last], rest[3 * last:]
    outs, (loss_ref, acc_h, acc_t, acc_r, blk_h, blk_t, blk_r, neg_acc, sems) = rest[:3 + last], rest[3 + last:]
    block = pl.program_id(0)
    accs = (acc_h, acc_t, acc_r)

    @pl.when(block == 0)
    def _():
        neg_acc[...] = jnp.zeros_like(neg_acc)
        loss_ref[...] = jnp.zeros_like(loss_ref)
        if last:
            copies = [pltpu.make_async_copy(src, acc, sems.at[slot]) for slot, (src, acc) in enumerate(zip(before, accs))]
            for copy in copies:
                copy.start()
            for copy in copies:
                copy.wait()
        else:
            rows = 16
            for acc in accs:
                def clear(step, carry, acc=acc):
                    acc[pl.ds(pl.multiple_of(step * rows, rows), rows), :] = jnp.zeros((rows, LANES), jnp.float32)
                    return carry

                lax.fori_loop(0, acc.shape[0] // rows, clear, 0)

    a_re, a_im = halves(a_ref)
    r_re, r_im = halves(r_ref)
    c_re, c_im = halves(c_ref)
    q_re = a_re * r_re - a_im * r_im
    q_im = a_re * r_im + a_im * r_re
    q_bf = qm_ref[...]
    m_mine = mm_ref[...]
    nt = (((1,), (1,)), ((), ()))
    score = lax.dot_general(q_bf, m_mine, nt, preferred_element_type=jnp.float32)
    score = score + lax.dot_general(qp_ref[...], mp_ref[...], nt, preferred_element_type=jnp.float32)
    lane = lax.broadcasted_iota(jnp.int32, score.shape, 1)
    score = jnp.where(lane < negs, score, -jnp.inf)
    pos = column(pm_ref[0] + pp_ref[0])
    weight = column(w_ref[0])
    low, high = score[:, :LANES], score[:, LANES:]
    top = jnp.maximum(pos, jnp.max(jnp.maximum(low, high), axis=1, keepdims=True))
    pos_exp = jnp.exp(pos - top)
    low_exp, high_exp = jnp.exp(low - top), jnp.exp(high - top)
    norm = pos_exp + jnp.sum(low_exp + high_exp, axis=1, keepdims=True)
    loss_ref[...] += jnp.sum(weight * (top + jnp.log(norm) - pos), axis=0, keepdims=True)
    alpha = weight * (pos_exp / norm - 1.0)
    scale = weight / norm
    beta = jnp.concatenate([(scale * low_exp).astype(jnp.bfloat16), (scale * high_exp).astype(jnp.bfloat16)], axis=1)
    nn = (((1,), (0,)), ((), ()))
    mixed = lax.dot_general(beta, m_mine, nn, preferred_element_type=jnp.float32)
    tn = (((0,), (0,)), ((), ()))
    neg_acc[...] += lax.dot_general(beta, q_bf, tn, preferred_element_type=jnp.float32)
    d_re = alpha * c_re + mixed[:, :LANES]
    d_im = alpha * c_im + mixed[:, LANES:]
    put_halves(blk_t, alpha * q_re, alpha * q_im)
    put_halves(blk_h, d_re * r_re + d_im * r_im, d_im * r_re - d_re * r_im)
    put_halves(blk_r, d_re * a_re + d_im * a_im, d_im * a_re - d_re * a_im)

    unroll = 16

    def some(step, carry):
        for sub in range(unroll):
            edge = step * unroll + sub
            here = pair_at(2 * edge)
            at_h, at_t, at_r = (pair_at(ref[0, 0, edge]) for ref in (head_ref, tail_ref, rel_ref))
            acc_h[at_h, :] = acc_h[at_h, :] + blk_h[here, :]
            acc_t[at_t, :] = acc_t[at_t, :] + blk_t[here, :]
            acc_r[at_r, :] = acc_r[at_r, :] + blk_r[here, :]
        return carry

    lax.fori_loop(0, BLOCK // unroll, some, 0)

    @pl.when(block == pl.num_programs(0) - 1)
    def _():
        put_halves(blk_t, neg_acc[:, :LANES], neg_acc[:, LANES:])
        small = 8

        def more(step, carry):
            for sub in range(small):
                row = step * small + sub
                at_t = pair_at(neg_ref[0, 0, row])
                acc_t[at_t, :] = acc_t[at_t, :] + blk_t[pair_at(2 * row), :]
            return carry

        lax.fori_loop(0, negs // small, more, 0)
        sources = list(accs)
        if last:
            half = acc_r.shape[0] // 2
            core = core_ref[0]
            sources[2:] = [acc_r.at[pl.ds(pl.multiple_of(at * half, 8), half)] for at in (core, 1 - core)]
        copies = [pltpu.make_async_copy(src, out, sems.at[slot]) for slot, (src, out) in enumerate(zip(sources, outs))]
        for copy in copies:
            copy.start()
        for copy in copies:
            copy.wait()


def smem_block(width):
    return pl.BlockSpec((1, 1, width), lambda b: (b, 0, 0), memory_space=pltpu.SMEM)


PAIRS = pl.BlockSpec((2 * BLOCK, LANES), lambda b: (b, 0))
WIDE = pl.BlockSpec((BLOCK, 2 * LANES), lambda b: (b, 0))
ROW = pl.BlockSpec((1, 1, BLOCK), lambda b: (b, 0, 0))
NEGS = pl.BlockSpec((2 * LANES, 2 * LANES), lambda b: (0, 0))
ANYWHERE = pl.BlockSpec(memory_space=pl.ANY)
SCALARS = pl.BlockSpec(memory_space=pltpu.SMEM)
PARAMS = dict(dimension_semantics=("arbitrary",), vmem_limit_bytes=VMEM_CAP)


def query_rows(core, ent, rel_mine, rel_other, head_ids, rel_ids):
    blocks = head_ids.shape[0]
    edges = blocks * BLOCK
    return pl.pallas_call(
        query_kernel,
        grid=(blocks,),
        in_specs=[SCALARS, smem_block(BLOCK), smem_block(BLOCK), ANYWHERE, ANYWHERE, ANYWHERE],
        out_specs=[PAIRS, PAIRS, WIDE],
        out_shape=[
            jax.ShapeDtypeStruct((2 * edges, LANES), jnp.float32),
            jax.ShapeDtypeStruct((2 * edges, LANES), jnp.float32),
            jax.ShapeDtypeStruct((edges, 2 * LANES), jnp.bfloat16),
        ],
        scratch_shapes=[
            pltpu.VMEM(ent.shape, jnp.float32),
            pltpu.VMEM((2 * rel_mine.shape[0], LANES), jnp.float32),
            pltpu.SemaphoreType.DMA((3,)),
        ],
        compiler_params=pltpu.CompilerParams(**PARAMS),
        cost_estimate=pl.CostEstimate(flops=100_000_000, bytes_accessed=80_000_000, transcendentals=0),
        name="query_rows",
    )(core, head_ids, rel_ids, ent, rel_mine, rel_other)


def tail_rows(table, tail_ids, neg_ids, a_rows, r_rows):
    blocks = tail_ids.shape[0]
    edges = blocks * BLOCK
    negs = neg_ids.shape[-1]
    return pl.pallas_call(
        functools.partial(tail_kernel, negs),
        grid=(blocks,),
        in_specs=[smem_block(BLOCK), SCALARS, PAIRS, PAIRS, ANYWHERE],
        out_specs=[PAIRS, ROW, NEGS],
        out_shape=[
            jax.ShapeDtypeStruct((2 * edges, LANES), jnp.float32),
            jax.ShapeDtypeStruct((blocks, 1, BLOCK), jnp.float32),
            jax.ShapeDtypeStruct((2 * LANES, 2 * LANES), jnp.bfloat16),
        ],
        scratch_shapes=[
            pltpu.VMEM(table.shape, jnp.bfloat16),
            pltpu.VMEM(table.shape, jnp.float32),
            pltpu.VMEM((4 * LANES, LANES), jnp.float32),
            pltpu.SemaphoreType.DMA,
        ],
        compiler_params=pltpu.CompilerParams(**PARAMS),
        cost_estimate=pl.CostEstimate(flops=100_000_000, bytes_accessed=60_000_000, transcendentals=0),
        name="tail_rows",
    )(tail_ids, neg_ids, a_rows, r_rows, table)


def bucket_grads(core, ids, neg_ids, rows, queries, scores, weight, negatives, before, ent_shape, rel_shape):
    blocks = ids[0].shape[0]
    last = before is not None
    before = before or ()
    half_shape = (rel_shape[0] // 2, LANES)
    shapes = [ent_shape, ent_shape] + ([half_shape, half_shape] if last else [rel_shape])
    return pl.pallas_call(
        functools.partial(grad_kernel, int(last), neg_ids.shape[-1]),
        grid=(blocks,),
        in_specs=[SCALARS] + [smem_block(BLOCK)] * 3 + [SCALARS] + [PAIRS] * 3 + [WIDE] * 2 + [ROW] * 3 + [NEGS] * 2
        + [ANYWHERE] * len(before),
        out_specs=[ANYWHERE] * len(shapes) + [pl.BlockSpec((1, LANES), lambda b: (0, 0))],
        out_shape=[jax.ShapeDtypeStruct(shape, jnp.float32) for shape in shapes + [(1, LANES)]],
        scratch_shapes=[
            pltpu.VMEM(ent_shape, jnp.float32),
            pltpu.VMEM(ent_shape, jnp.float32),
            pltpu.VMEM(rel_shape, jnp.float32),
            pltpu.VMEM((2 * BLOCK, LANES), jnp.float32),
            pltpu.VMEM((2 * BLOCK, LANES), jnp.float32),
            pltpu.VMEM((2 * BLOCK, LANES), jnp.float32),
            pltpu.VMEM((2 * LANES, 2 * LANES), jnp.float32),
            pltpu.SemaphoreType.DMA((4,)),
        ],
        compiler_params=pltpu.CompilerParams(**PARAMS),
        cost_estimate=pl.CostEstimate(flops=300_000_000, bytes_accessed=200_000_000, transcendentals=2_000_000),
        name="bucket_grads",
    )(core, *ids, neg_ids, *rows, *queries, *scores, weight, *negatives, *before)


def square_kernel(one_ref, two_ref, *rest):
    g_ref, sum_ref = rest[-2:]
    g_ref[...] = one_ref[...] + two_ref[...]
    real, imag = halves(g_ref)
    sum_ref[0] = jnp.sum((real * real + imag * imag).T, axis=0, keepdims=True)


def step_kernel(rate, dim, par_ref, g_ref, state_ref, sm_ref, sp_ref, out_ref, new_ref, *bf_refs):
    state = state_ref[0] + (sm_ref[0] + sp_ref[0]) / dim
    new_ref[0] = state
    scale = column(rate / jnp.sqrt(state + ADA_EPS))
    p_re, p_im = halves(par_ref)
    g_re, g_im = halves(g_ref)
    put_halves(out_ref, p_re - g_re * scale, p_im - g_im * scale)
    for ref in bf_refs:
        ref[...] = out_ref[...].astype(jnp.bfloat16)


def adagrad(param, state, one, two, rate, dim, swap, with_bf, after=()):
    blocks = state.shape[0]
    pairs = pl.BlockSpec((2 * WIDE_ROWS, LANES), lambda b: (b, 0))
    row = pl.BlockSpec((1, 1, WIDE_ROWS), lambda b: (b, 0, 0))
    wide = jax.ShapeDtypeStruct(param.shape, jnp.float32)
    narrow = jax.ShapeDtypeStruct(state.shape, jnp.float32)
    params = pltpu.CompilerParams(dimension_semantics=("arbitrary",))
    size = 4 * param.size
    grad, sums = pl.pallas_call(
        square_kernel,
        grid=(blocks,),
        in_specs=[pairs, pairs] + [ANYWHERE] * len(after),
        out_specs=[pairs, row],
        out_shape=[wide, narrow],
        compiler_params=params,
        cost_estimate=pl.CostEstimate(flops=4 * param.size, bytes_accessed=3 * size, transcendentals=0),
        name="square_sums",
    )(one, two, *after)
    sums_peer = lax.ppermute(sums, "data", swap)
    bf_shapes = [jax.ShapeDtypeStruct(param.shape, jnp.bfloat16)] if with_bf else []
    return pl.pallas_call(
        functools.partial(step_kernel, rate, dim),
        grid=(blocks,),
        in_specs=[pairs, pairs, row, row, row],
        out_specs=[pairs, row] + [pairs] * len(bf_shapes),
        out_shape=[wide, narrow] + bf_shapes,
        compiler_params=params,
        cost_estimate=pl.CostEstimate(flops=4 * param.size, bytes_accessed=3 * size, transcendentals=0),
        name="adagrad_step",
    )(param, grad, state, sums, sums_peer)


def solution(mesh):
    ent_size = mesh.shape["ent"]
    data_size = mesh.shape["data"]
    swap = [(src, data_size - 1 - src) for src in range(data_size)]
    core_swap = [(src, src ^ 1) for src in range(ent_size)]
    chip_swap = [(src, src ^ 2) for src in range(ent_size)]

    def device_epoch(ent_table, ada_state, rel_table, head_idx, tail_idx, rel_idx, edge_mask, neg_idx):
        _, dim = ent_table.shape
        rel_rows = rel_table.shape[0]
        edge_count = head_idx.shape[-1]
        negs = neg_idx.shape[-1]
        part = lax.axis_index("data")
        core = lax.rem(lax.axis_index("ent"), 2)
        core_at = core[None]
        ent, table = split_columns(ent_table, part, True)
        rel = split_columns(rel_table, part, False)[0]
        ent_shape, rel_shape = ent.shape, rel.shape
        rel_mine = lax.dynamic_slice_in_dim(rel, core * rel_rows, rel_rows, axis=0)
        rel_other = lax.dynamic_slice_in_dim(rel, (1 - core) * rel_rows, rel_rows, axis=0)
        state = ada_state.reshape(-1, 1, WIDE_ROWS)
        rel_state = jnp.zeros((pl.cdiv(rel_rows // 2, WIDE_ROWS), 1, WIDE_ROWS), jnp.float32)

        local = jnp.concatenate(
            [2 * head_idx[0, 0], 2 * tail_idx[0, 0], 2 * rel_idx[0, 0], edge_mask[0, 0], 2 * neg_idx[0, 0]], axis=1)
        both = lax.all_gather(local, "data")
        blocks = edge_count // BLOCK

        def field(slot, bucket, round_idx):
            return both[bucket, round_idx, slot * edge_count:(slot + 1) * edge_count].reshape(blocks, 1, BLOCK)

        losses = []
        for round_idx in range(ent_size):
            if round_idx:
                fetch = [((dest + round_idx) % ent_size, dest) for dest in range(ent_size)]
                table = lax.ppermute(table, "ent", fetch)
            ids = [[field(slot, bucket, round_idx) for slot in range(3)] for bucket in range(data_size)]
            asked = [query_rows(core_at, ent, rel_mine, rel_other, ids[bucket][0], ids[bucket][2]) for bucket in range(data_size)]
            before = None
            sums = []
            for bucket in range(data_size):
                a_rows, r_rows, q_mine = asked[bucket]
                q_peer = lax.ppermute(q_mine, "data", swap)
                neg_ids = both[bucket, round_idx, 4 * edge_count:].reshape(1, 1, negs)
                c_rows, p_mine, m_mine = tail_rows(table, ids[bucket][1], neg_ids, a_rows, r_rows)
                m_peer = lax.ppermute(m_mine, "data", swap)
                p_peer = lax.ppermute(p_mine, "data", swap)
                *before, loss = bucket_grads(
                    core_at, ids[bucket], neg_ids, (a_rows, r_rows, c_rows), (q_mine, q_peer), (p_mine, p_peer),
                    field(3, bucket, round_idx).astype(jnp.float32), (m_mine, m_peer), before, ent_shape, rel_shape)
                sums.append(loss[0, 0])
            g_head, g_tail, keep, give = before
            if round_idx:
                back = [(src, (src + round_idx) % ent_size) for src in range(ent_size)]
                g_tail = lax.ppermute(g_tail, "ent", back)
            chip_sum = keep + lax.ppermute(give, "ent", core_swap)
            chip_other = lax.ppermute(chip_sum, "ent", chip_swap)
            ent, state, table = adagrad(ent, state, g_head, g_tail, LEARN_ENT, dim, swap, True)
            rel_mine, rel_state = adagrad(rel_mine, rel_state, chip_sum, chip_other, LEARN_REL, dim, swap, False, (state,))
            if round_idx < ent_size - 1:
                rel_other = lax.ppermute(rel_mine, "ent", core_swap)
            losses.append(jnp.where(part == 0, sums[0], sums[1]) / edge_count)

        def join(half):
            flipped = flip_half(half, dim)
            peer = lax.ppermute(flipped, "data", swap)
            first = jnp.where(part == 0, flipped, peer)
            second = jnp.where(part == 0, peer, flipped)
            return jnp.stack([first, second], axis=1).reshape(dim, -1)

        ent_out = join(ent).T
        rel_cols = join(rel_mine)
        rel_cols_other = lax.ppermute(rel_cols, "ent", core_swap)
        rel_out = jnp.concatenate(
            [jnp.where(core == 0, rel_cols, rel_cols_other), jnp.where(core == 0, rel_cols_other, rel_cols)], axis=1).T
        return ent_out, state.reshape(-1), rel_out, jnp.stack(losses)[None, None, :]

    ent_spec = P(("sweep", "ent"), None)
    row_spec = P(("sweep", "ent"))
    rel_spec = P("sweep", None)
    edge_spec = P(("sweep", "ent"), "data", None, None)
    loss_spec = P(("sweep", "ent"), "data", None)
    return jax.shard_map(
        device_epoch, mesh=mesh,
        in_specs=(ent_spec, row_spec, rel_spec, edge_spec, edge_spec, edge_spec, edge_spec, edge_spec),
        out_specs=(ent_spec, row_spec, rel_spec, loss_spec),
        check_vma=False)
```

```python
import functools

import jax
import jax.numpy as jnp
from jax import lax
from jax.experimental import pallas as pl
from jax.experimental.pallas import tpu as pltpu
from jax.sharding import PartitionSpec as P


LEARN_ENT = 0.1
LEARN_REL = 0.05
ADA_EPS = 1e-6
LANES = 128
BLOCK = 256
WIDE_ROWS = 512
VMEM_CAP = 66_000_000


def pair_at(row):
    return pl.ds(pl.multiple_of(row, 2), 2)


def halves(ref):
    count = ref.shape[0] // 2
    return ref[pl.ds(0, count, stride=2), :], ref[pl.ds(1, count, stride=2), :]


def put_halves(ref, real, imag):
    count = ref.shape[0] // 2
    ref[pl.ds(0, count, stride=2), :] = real
    ref[pl.ds(1, count, stride=2), :] = imag


def split_kernel(width, part_ref, in_ref, out_ref, *bf_refs):
    second = part_ref[0] != 0
    lane = lax.broadcasted_iota(jnp.int32, (out_ref.shape[0] // 2, LANES), 1)

    def pick(start):
        last = in_ref.shape[0] - LANES
        shift = max(start - last, 0)
        rows = in_ref[pl.ds(start - shift, LANES), :].T
        if shift:
            rows = pltpu.roll(rows, LANES - shift, 1)
        return jnp.where(lane < width, rows, 0.0)

    real = jnp.where(second, pick(width), pick(0))
    imag = jnp.where(second, pick(3 * width), pick(2 * width))
    put_halves(out_ref, real, imag)
    for ref in bf_refs:
        ref[...] = out_ref[...].astype(jnp.bfloat16)


def split_columns(table, part, with_bf):
    rows, dim = table.shape
    pairs = pl.BlockSpec((2 * WIDE_ROWS, LANES), lambda b: (b, 0))
    kinds = [jnp.float32, jnp.bfloat16] if with_bf else [jnp.float32]
    return pl.pallas_call(
        functools.partial(split_kernel, dim // 4),
        grid=(pl.cdiv(rows, WIDE_ROWS),),
        in_specs=[pl.BlockSpec(memory_space=pltpu.SMEM), pl.BlockSpec((dim, WIDE_ROWS), lambda b: (0, b))],
        out_specs=[pairs] * len(kinds),
        out_shape=[jax.ShapeDtypeStruct((2 * rows, LANES), kind) for kind in kinds],
        compiler_params=pltpu.CompilerParams(dimension_semantics=("arbitrary",)),
        cost_estimate=pl.CostEstimate(flops=20_000_000, bytes_accessed=45_000_000, transcendentals=0),
        name="split_columns",
    )(part[None], table.T)


def flip_kernel(in_ref, out_ref):
    real, imag = halves(in_ref)
    width = out_ref.shape[0] // 2
    out_ref[pl.ds(0, width), :] = real.T[:width, :]
    out_ref[pl.ds(width, width), :] = imag.T[:width, :]


def flip_half(half, dim):
    rows = half.shape[0] // 2
    return pl.pallas_call(
        flip_kernel,
        grid=(pl.cdiv(rows, WIDE_ROWS),),
        in_specs=[pl.BlockSpec((2 * WIDE_ROWS, LANES), lambda b: (b, 0))],
        out_specs=pl.BlockSpec((dim // 2, WIDE_ROWS), lambda b: (0, b)),
        out_shape=jax.ShapeDtypeStruct((dim // 2, rows), jnp.float32),
        compiler_params=pltpu.CompilerParams(dimension_semantics=("arbitrary",)),
        cost_estimate=pl.CostEstimate(flops=20_000_000, bytes_accessed=30_000_000, transcendentals=0),
        name="flip_half",
    )(half)


def query_kernel(core_ref, head_ref, rel_ref, ent_hbm, relm_hbm, relo_hbm, a_ref, r_ref, q_ref, ent_v, rel_v, sems):
    @pl.when(pl.program_id(0) == 0)
    def _():
        half = relm_hbm.shape[0]
        core = core_ref[0]
        mine = pl.ds(pl.multiple_of(core * half, 8), half)
        other = pl.ds(pl.multiple_of((1 - core) * half, 8), half)
        copies = [
            pltpu.make_async_copy(ent_hbm, ent_v, sems.at[0]),
            pltpu.make_async_copy(relm_hbm, rel_v.at[mine], sems.at[1]),
            pltpu.make_async_copy(relo_hbm, rel_v.at[other], sems.at[2]),
        ]
        for copy in copies:
            copy.start()
        for copy in copies:
            copy.wait()

    unroll = 32

    def some(step, carry):
        for sub in range(unroll):
            edge = step * unroll + sub
            a_ref[pair_at(2 * edge), :] = ent_v[pair_at(head_ref[0, 0, edge]), :]
            r_ref[pair_at(2 * edge), :] = rel_v[pair_at(rel_ref[0, 0, edge]), :]
        return carry

    lax.fori_loop(0, BLOCK // unroll, some, 0)
    a_re, a_im = halves(a_ref)
    r_re, r_im = halves(r_ref)
    q_ref[:, :LANES] = (a_re * r_re - a_im * r_im).astype(jnp.bfloat16)
    q_ref[:, LANES:] = (a_re * r_im + a_im * r_re).astype(jnp.bfloat16)


def tail_kernel(negs, tail_ref, neg_ref, a_ref, r_ref, tab_hbm, c_ref, p_ref, m_ref, tab_bf, tab_v, neg_v, sem):
    @pl.when(pl.program_id(0) == 0)
    def _():
        copy = pltpu.make_async_copy(tab_hbm, tab_bf, sem)
        copy.start()
        copy.wait()
        rows = 512

        def widen(step, carry):
            at = pl.ds(pl.multiple_of(step * rows, rows), rows)
            tab_v[at, :] = tab_bf[at, :].astype(jnp.float32)
            return carry

        lax.fori_loop(0, tab_v.shape[0] // rows, widen, 0)
        neg_v[...] = jnp.zeros_like(neg_v)
        small = 8

        def pick(step, carry):
            for sub in range(small):
                row = step * small + sub
                neg_v[pair_at(2 * row), :] = tab_v[pair_at(neg_ref[0, 0, row]), :]
            return carry

        lax.fori_loop(0, negs // small, pick, 0)
        m_re, m_im = halves(neg_v)
        m_ref[:, :LANES] = m_re.astype(jnp.bfloat16)
        m_ref[:, LANES:] = m_im.astype(jnp.bfloat16)

    unroll = 32

    def some(step, carry):
        for sub in range(unroll):
            edge = step * unroll + sub
            c_ref[pair_at(2 * edge), :] = tab_v[pair_at(tail_ref[0, 0, edge]), :]
        return carry

    lax.fori_loop(0, BLOCK // unroll, some, 0)
    a_re, a_im = halves(a_ref)
    r_re, r_im = halves(r_ref)
    c_re, c_im = halves(c_ref)
    prod = (a_re * r_re - a_im * r_im) * c_re + (a_re * r_im + a_im * r_re) * c_im
    p_ref[0] = jnp.sum(prod.T, axis=0, keepdims=True)


def column(row):
    return jnp.broadcast_to(row, (LANES, row.shape[-1])).T


def grad_kernel(
    last, negs,
    core_ref, head_ref, rel_ref, a_ref, r_ref, c_ref, qm_ref, qp_ref, pm_ref, pp_ref, w_ref, mm_ref, mp_ref,
    *rest,
):
    before, rest = rest[:2 * last], rest[2 * last:]
    outs, (t_ref, n_ref, loss_ref, acc_h, acc_r, blk_h, blk_r, neg_acc, sems) = rest[:2 + last], rest[2 + last:]
    block = pl.program_id(0)
    accs = (acc_h, acc_r)

    @pl.when(block == 0)
    def _():
        neg_acc[...] = jnp.zeros_like(neg_acc)
        loss_ref[...] = jnp.zeros_like(loss_ref)
        if last:
            copies = [pltpu.make_async_copy(src, acc, sems.at[slot]) for slot, (src, acc) in enumerate(zip(before, accs))]
            for copy in copies:
                copy.start()
            for copy in copies:
                copy.wait()
        else:
            for acc in accs:
                rows = max(size for size in range(8, 513, 8) if acc.shape[0] % size == 0)

                def clear(step, carry, acc=acc, rows=rows):
                    acc[pl.ds(pl.multiple_of(step * rows, rows), rows), :] = jnp.zeros((rows, LANES), jnp.float32)
                    return carry

                lax.fori_loop(0, acc.shape[0] // rows, clear, 0)

    a_re, a_im = halves(a_ref)
    r_re, r_im = halves(r_ref)
    c_re, c_im = halves(c_ref)
    q_re = a_re * r_re - a_im * r_im
    q_im = a_re * r_im + a_im * r_re
    q_bf = qm_ref[...]
    m_mine = mm_ref[...]
    nt = (((1,), (1,)), ((), ()))
    score = lax.dot_general(q_bf, m_mine, nt, preferred_element_type=jnp.float32)
    score = score + lax.dot_general(qp_ref[...], mp_ref[...], nt, preferred_element_type=jnp.float32)
    lane = lax.broadcasted_iota(jnp.int32, score.shape, 1)
    score = jnp.where(lane < negs, score, -jnp.inf)
    pos = column(pm_ref[0] + pp_ref[0])
    weight = column(w_ref[0])
    low, high = score[:, :LANES], score[:, LANES:]
    top = jnp.maximum(pos, jnp.max(jnp.maximum(low, high), axis=1, keepdims=True))
    pos_exp = jnp.exp(pos - top)
    low_exp, high_exp = jnp.exp(low - top), jnp.exp(high - top)
    norm = pos_exp + jnp.sum(low_exp + high_exp, axis=1, keepdims=True)
    loss_ref[...] += jnp.sum(weight * (top + jnp.log(norm) - pos), axis=0, keepdims=True)
    alpha = weight * (pos_exp / norm - 1.0)
    scale = weight / norm
    beta = jnp.concatenate([(scale * low_exp).astype(jnp.bfloat16), (scale * high_exp).astype(jnp.bfloat16)], axis=1)
    nn = (((1,), (0,)), ((), ()))
    mixed = lax.dot_general(beta, m_mine, nn, preferred_element_type=jnp.float32)
    tn = (((0,), (0,)), ((), ()))
    neg_acc[...] += lax.dot_general(beta, q_bf, tn, preferred_element_type=jnp.float32)
    d_re = alpha * c_re + mixed[:, :LANES]
    d_im = alpha * c_im + mixed[:, LANES:]
    put_halves(t_ref, alpha * q_re, alpha * q_im)
    put_halves(blk_h, d_re * r_re + d_im * r_im, d_im * r_re - d_re * r_im)
    put_halves(blk_r, d_re * a_re + d_im * a_im, d_im * a_re - d_re * a_im)

    unroll = 16

    def some(step, carry):
        for sub in range(unroll):
            edge = step * unroll + sub
            here = pair_at(2 * edge)
            at_h, at_r = (pair_at(ref[0, 0, edge]) for ref in (head_ref, rel_ref))
            acc_h[at_h, :] = acc_h[at_h, :] + blk_h[here, :]
            acc_r[at_r, :] = acc_r[at_r, :] + blk_r[here, :]
        return carry

    lax.fori_loop(0, BLOCK // unroll, some, 0)

    @pl.when(block == pl.num_programs(0) - 1)
    def _():
        put_halves(n_ref, neg_acc[:, :LANES], neg_acc[:, LANES:])
        sources = list(accs)
        if last:
            half = acc_r.shape[0] // 2
            core = core_ref[0]
            sources[1:] = [acc_r.at[pl.ds(pl.multiple_of(at * half, 8), half)] for at in (core, 1 - core)]
        copies = [pltpu.make_async_copy(src, out, sems.at[slot]) for slot, (src, out) in enumerate(zip(sources, outs))]
        for copy in copies:
            copy.start()
        for copy in copies:
            copy.wait()


def smem_block(width):
    return pl.BlockSpec((1, 1, width), lambda b: (b, 0, 0), memory_space=pltpu.SMEM)


PAIRS = pl.BlockSpec((2 * BLOCK, LANES), lambda b: (b, 0))
WIDE = pl.BlockSpec((BLOCK, 2 * LANES), lambda b: (b, 0))
ROW = pl.BlockSpec((1, 1, BLOCK), lambda b: (b, 0, 0))
NEGS = pl.BlockSpec((2 * LANES, 2 * LANES), lambda b: (0, 0))
ANYWHERE = pl.BlockSpec(memory_space=pl.ANY)
SCALARS = pl.BlockSpec(memory_space=pltpu.SMEM)
PARAMS = dict(dimension_semantics=("arbitrary",), vmem_limit_bytes=VMEM_CAP)


def query_rows(core, ent, rel_mine, rel_other, head_ids, rel_ids):
    blocks = head_ids.shape[0]
    edges = blocks * BLOCK
    return pl.pallas_call(
        query_kernel,
        grid=(blocks,),
        in_specs=[SCALARS, smem_block(BLOCK), smem_block(BLOCK), ANYWHERE, ANYWHERE, ANYWHERE],
        out_specs=[PAIRS, PAIRS, WIDE],
        out_shape=[
            jax.ShapeDtypeStruct((2 * edges, LANES), jnp.float32),
            jax.ShapeDtypeStruct((2 * edges, LANES), jnp.float32),
            jax.ShapeDtypeStruct((edges, 2 * LANES), jnp.bfloat16),
        ],
        scratch_shapes=[
            pltpu.VMEM(ent.shape, jnp.float32),
            pltpu.VMEM((2 * rel_mine.shape[0], LANES), jnp.float32),
            pltpu.SemaphoreType.DMA((3,)),
        ],
        compiler_params=pltpu.CompilerParams(**PARAMS),
        cost_estimate=pl.CostEstimate(flops=100_000_000, bytes_accessed=80_000_000, transcendentals=0),
        name="query_rows",
    )(core, head_ids, rel_ids, ent, rel_mine, rel_other)


def tail_rows(table, tail_ids, neg_ids, a_rows, r_rows):
    blocks = tail_ids.shape[0]
    edges = blocks * BLOCK
    negs = neg_ids.shape[-1]
    return pl.pallas_call(
        functools.partial(tail_kernel, negs),
        grid=(blocks,),
        in_specs=[smem_block(BLOCK), SCALARS, PAIRS, PAIRS, ANYWHERE],
        out_specs=[PAIRS, ROW, NEGS],
        out_shape=[
            jax.ShapeDtypeStruct((2 * edges, LANES), jnp.float32),
            jax.ShapeDtypeStruct((blocks, 1, BLOCK), jnp.float32),
            jax.ShapeDtypeStruct((2 * LANES, 2 * LANES), jnp.bfloat16),
        ],
        scratch_shapes=[
            pltpu.VMEM(table.shape, jnp.bfloat16),
            pltpu.VMEM(table.shape, jnp.float32),
            pltpu.VMEM((4 * LANES, LANES), jnp.float32),
            pltpu.SemaphoreType.DMA,
        ],
        compiler_params=pltpu.CompilerParams(**PARAMS),
        cost_estimate=pl.CostEstimate(flops=100_000_000, bytes_accessed=60_000_000, transcendentals=0),
        name="tail_rows",
    )(tail_ids, neg_ids, a_rows, r_rows, table)


def bucket_grads(core, ids, negs, rows, queries, scores, weight, negatives, before, ent_shape, rel_shape):
    blocks = ids[0].shape[0]
    last = before is not None
    before = before or ()
    half_shape = (rel_shape[0] // 2, LANES)
    shapes = [ent_shape] + ([half_shape, half_shape] if last else [rel_shape])
    neg_pairs = (4 * LANES, LANES)
    flat = lambda b: (0, 0)
    return pl.pallas_call(
        functools.partial(grad_kernel, int(last), negs),
        grid=(blocks,),
        in_specs=[SCALARS] + [smem_block(BLOCK)] * 2 + [PAIRS] * 3 + [WIDE] * 2 + [ROW] * 3 + [NEGS] * 2
        + [ANYWHERE] * len(before),
        out_specs=[ANYWHERE] * len(shapes) + [PAIRS, pl.BlockSpec(neg_pairs, flat), pl.BlockSpec((1, LANES), flat)],
        out_shape=[
            jax.ShapeDtypeStruct(shape, jnp.float32)
            for shape in shapes + [(2 * blocks * BLOCK, LANES), neg_pairs, (1, LANES)]
        ],
        scratch_shapes=[
            pltpu.VMEM(ent_shape, jnp.float32),
            pltpu.VMEM(rel_shape, jnp.float32),
            pltpu.VMEM((2 * BLOCK, LANES), jnp.float32),
            pltpu.VMEM((2 * BLOCK, LANES), jnp.float32),
            pltpu.VMEM((2 * LANES, 2 * LANES), jnp.float32),
            pltpu.SemaphoreType.DMA((3,)),
        ],
        compiler_params=pltpu.CompilerParams(**PARAMS),
        cost_estimate=pl.CostEstimate(flops=300_000_000, bytes_accessed=200_000_000, transcendentals=2_000_000),
        name="bucket_grads",
    )(core, *ids, *rows, *queries, *scores, weight, *negatives, *before)


def add_kernel(negs, tail_ref, neg_ref, rows_ref, n_ref, base_hbm, g_hbm, *rest):
    sum_refs, (acc, sem) = rest[:-2], rest[-2:]
    block = pl.program_id(0)

    @pl.when(block == 0)
    def _():
        copy = pltpu.make_async_copy(base_hbm, acc, sem)
        copy.start()
        copy.wait()
        small = 8

        def more(step, carry):
            for sub in range(small):
                row = step * small + sub
                at = pair_at(neg_ref[0, 0, row])
                acc[at, :] = acc[at, :] + n_ref[pair_at(2 * row), :]
            return carry

        lax.fori_loop(0, negs // small, more, 0)

    unroll = 16

    def some(step, carry):
        for sub in range(unroll):
            edge = step * unroll + sub
            at = pair_at(tail_ref[0, 0, edge])
            acc[at, :] = acc[at, :] + rows_ref[pair_at(2 * edge), :]
        return carry

    lax.fori_loop(0, BLOCK // unroll, some, 0)

    @pl.when(block == pl.num_programs(0) - 1)
    def _():
        copy = pltpu.make_async_copy(acc, g_hbm, sem)
        copy.start()
        for sum_ref in sum_refs:
            width = sum_ref.shape[-1]

            def square(step, carry):
                start = pl.multiple_of(step * 2 * width, 2 * width)
                real = acc[pl.ds(start, width, stride=2), :]
                imag = acc[pl.ds(start + 1, width, stride=2), :]
                sum_ref[step] = jnp.sum((real * real + imag * imag).T, axis=0, keepdims=True)
                return carry

            lax.fori_loop(0, sum_ref.shape[0], square, 0)
        copy.wait()


def add_rows(base, tail_ids, neg_ids, rows, neg_rows, sum_shape):
    blocks = tail_ids.shape[0]
    sums = [] if sum_shape is None else [sum_shape]
    return pl.pallas_call(
        functools.partial(add_kernel, neg_ids.shape[-1]),
        grid=(blocks,),
        in_specs=[smem_block(BLOCK), SCALARS, PAIRS, pl.BlockSpec(neg_rows.shape, lambda b: (0, 0)), ANYWHERE],
        out_specs=[ANYWHERE] + [pl.BlockSpec(shape, lambda b: (0, 0, 0)) for shape in sums],
        out_shape=[jax.ShapeDtypeStruct(shape, jnp.float32) for shape in [base.shape] + sums],
        scratch_shapes=[pltpu.VMEM(base.shape, jnp.float32), pltpu.SemaphoreType.DMA],
        compiler_params=pltpu.CompilerParams(**PARAMS),
        cost_estimate=pl.CostEstimate(flops=100_000_000, bytes_accessed=100_000_000, transcendentals=0),
        name="add_rows",
    )(tail_ids, neg_ids, rows, neg_rows, base)


def square_kernel(one_ref, two_ref, *rest):
    g_ref, sum_ref = rest[-2:]
    g_ref[...] = one_ref[...] + two_ref[...]
    real, imag = halves(g_ref)
    sum_ref[0] = jnp.sum((real * real + imag * imag).T, axis=0, keepdims=True)


def step_kernel(rate, dim, par_ref, g_ref, state_ref, sm_ref, sp_ref, out_ref, new_ref, *bf_refs):
    state = state_ref[0] + (sm_ref[0] + sp_ref[0]) / dim
    new_ref[0] = state
    scale = column(rate / jnp.sqrt(state + ADA_EPS))
    p_re, p_im = halves(par_ref)
    g_re, g_im = halves(g_ref)
    put_halves(out_ref, p_re - g_re * scale, p_im - g_im * scale)
    for ref in bf_refs:
        ref[...] = out_ref[...].astype(jnp.bfloat16)


PAIR_ROWS = pl.BlockSpec((2 * WIDE_ROWS, LANES), lambda b: (b, 0))
WIDE_ROW = pl.BlockSpec((1, 1, WIDE_ROWS), lambda b: (b, 0, 0))


def square_sums(one, two, blocks, after):
    return pl.pallas_call(
        square_kernel,
        grid=(blocks,),
        in_specs=[PAIR_ROWS, PAIR_ROWS] + [ANYWHERE] * len(after),
        out_specs=[PAIR_ROWS, WIDE_ROW],
        out_shape=[
            jax.ShapeDtypeStruct(one.shape, jnp.float32),
            jax.ShapeDtypeStruct((blocks, 1, WIDE_ROWS), jnp.float32),
        ],
        compiler_params=pltpu.CompilerParams(dimension_semantics=("arbitrary",)),
        cost_estimate=pl.CostEstimate(flops=4 * one.size, bytes_accessed=12 * one.size, transcendentals=0),
        name="square_sums",
    )(one, two, *after)


def adagrad_step(param, state, grad, sums, rate, dim, swap, with_bf):
    sums_peer = lax.ppermute(sums, "data", swap)
    kinds = [jnp.float32, jnp.bfloat16] if with_bf else [jnp.float32]
    wide = [jax.ShapeDtypeStruct(param.shape, kind) for kind in kinds]
    return pl.pallas_call(
        functools.partial(step_kernel, rate, dim),
        grid=(state.shape[0],),
        in_specs=[PAIR_ROWS, PAIR_ROWS, WIDE_ROW, WIDE_ROW, WIDE_ROW],
        out_specs=[PAIR_ROWS, WIDE_ROW] + [PAIR_ROWS] * (len(kinds) - 1),
        out_shape=[wide[0], jax.ShapeDtypeStruct(state.shape, jnp.float32)] + wide[1:],
        compiler_params=pltpu.CompilerParams(dimension_semantics=("arbitrary",)),
        cost_estimate=pl.CostEstimate(flops=4 * param.size, bytes_accessed=12 * param.size, transcendentals=0),
        name="adagrad_step",
    )(param, grad, state, sums, sums_peer)


def join_kernel(part_ref, mine_ref, peer_ref, out_ref):
    second = part_ref[0] != 0
    width = mine_ref.shape[0] // 2
    for side in range(2):
        mine, peer = (ref[pl.ds(side * width, width), :] for ref in (mine_ref, peer_ref))
        out_ref[pl.ds(2 * side * width, width), :] = jnp.where(second, peer, mine)
        out_ref[pl.ds((2 * side + 1) * width, width), :] = jnp.where(second, mine, peer)


def join_columns(part, mine, peer):
    width, rows = mine.shape
    half = pl.BlockSpec((width, WIDE_ROWS), lambda b: (0, b))
    return pl.pallas_call(
        join_kernel,
        grid=(pl.cdiv(rows, WIDE_ROWS),),
        in_specs=[SCALARS, half, half],
        out_specs=pl.BlockSpec((2 * width, WIDE_ROWS), lambda b: (0, b)),
        out_shape=jax.ShapeDtypeStruct((2 * width, rows), jnp.float32),
        compiler_params=pltpu.CompilerParams(dimension_semantics=("arbitrary",)),
        cost_estimate=pl.CostEstimate(flops=mine.size, bytes_accessed=16 * mine.size, transcendentals=0),
        name="join_columns",
    )(part[None], mine, peer)


def solution(mesh):
    ent_size = mesh.shape["ent"]
    data_size = mesh.shape["data"]
    swap = [(src, data_size - 1 - src) for src in range(data_size)]
    core_swap = [(src, src ^ 1) for src in range(ent_size)]
    chip_swap = [(src, src ^ 2) for src in range(ent_size)]

    def device_epoch(ent_table, ada_state, rel_table, head_idx, tail_idx, rel_idx, edge_mask, neg_idx):
        _, dim = ent_table.shape
        rel_rows = rel_table.shape[0]
        edge_count = head_idx.shape[-1]
        negs = neg_idx.shape[-1]
        part = lax.axis_index("data")
        core = lax.rem(lax.axis_index("ent"), 2)
        core_at = core[None]
        ent, table = split_columns(ent_table, part, True)
        rel = split_columns(rel_table, part, False)[0]
        ent_shape, rel_shape = ent.shape, rel.shape
        rel_mine = lax.dynamic_slice_in_dim(rel, core * rel_rows, rel_rows, axis=0)
        rel_other = lax.dynamic_slice_in_dim(rel, (1 - core) * rel_rows, rel_rows, axis=0)
        state = ada_state.reshape(-1, 1, WIDE_ROWS)
        rel_state = jnp.zeros((pl.cdiv(rel_rows // 2, WIDE_ROWS), 1, WIDE_ROWS), jnp.float32)

        local = jnp.concatenate(
            [2 * head_idx[0, 0], 2 * tail_idx[0, 0], 2 * rel_idx[0, 0], edge_mask[0, 0], 2 * neg_idx[0, 0]], axis=1)
        both = lax.all_gather(local, "data")
        blocks = edge_count // BLOCK

        def field(slot, bucket, round_idx):
            return both[bucket, round_idx, slot * edge_count:(slot + 1) * edge_count].reshape(blocks, 1, BLOCK)

        def owned(round_idx):
            mine = jnp.concatenate(
                [both[:, round_idx, edge_count:2 * edge_count], both[:, round_idx, 4 * edge_count:]], axis=1)
            if round_idx:
                mine = lax.ppermute(mine, "ent", [(src, (src + round_idx) % ent_size) for src in range(ent_size)])
            return [
                (mine[bucket, :edge_count].reshape(blocks, 1, BLOCK), mine[bucket, edge_count:].reshape(1, 1, negs))
                for bucket in range(data_size)
            ]

        losses = []
        for round_idx in range(ent_size):
            if round_idx:
                fetch = [((dest + round_idx) % ent_size, dest) for dest in range(ent_size)]
                table = lax.ppermute(table, "ent", fetch)
            ids = [[field(slot, bucket, round_idx) for slot in range(3)] for bucket in range(data_size)]
            asked = [query_rows(core_at, ent, rel_mine, rel_other, ids[bucket][0], ids[bucket][2]) for bucket in range(data_size)]
            back = [(src, (src + round_idx) % ent_size) for src in range(ent_size)]
            targets = owned(round_idx)
            before = None
            sums, returned = [], []
            for bucket in range(data_size):
                a_rows, r_rows, q_mine = asked[bucket]
                q_peer = lax.ppermute(q_mine, "data", swap)
                neg_ids = both[bucket, round_idx, 4 * edge_count:].reshape(1, 1, negs)
                c_rows, p_mine, m_mine = tail_rows(table, ids[bucket][1], neg_ids, a_rows, r_rows)
                m_peer = lax.ppermute(m_mine, "data", swap)
                p_peer = lax.ppermute(p_mine, "data", swap)
                *before, t_rows, n_rows, loss = bucket_grads(
                    core_at, (ids[bucket][0], ids[bucket][2]), negs, (a_rows, r_rows, c_rows), (q_mine, q_peer),
                    (p_mine, p_peer), field(3, bucket, round_idx).astype(jnp.float32), (m_mine, m_peer), before,
                    ent_shape, rel_shape)
                sums.append(loss[0, 0])
                if round_idx:
                    t_rows = lax.ppermute(t_rows, "ent", back)
                    n_rows = lax.ppermute(n_rows, "ent", back)
                returned.append((t_rows, n_rows))
            g_ent, keep, give = before
            chip_sum = keep + lax.ppermute(give, "ent", core_swap)
            chip_other = lax.ppermute(chip_sum, "ent", chip_swap)
            for bucket in range(data_size):
                shape = state.shape if bucket == data_size - 1 else None
                g_ent, *ent_sums = add_rows(g_ent, *targets[bucket], *returned[bucket], shape)
            ent, state, table = adagrad_step(ent, state, g_ent, ent_sums[0], LEARN_ENT, dim, swap, True)
            after = state
            if round_idx == ent_size - 1:
                ent_cols = after = flip_half(ent, dim)
                ent_cols_peer = lax.ppermute(ent_cols, "data", swap)
            g_rel, rel_sums = square_sums(chip_sum, chip_other, rel_state.shape[0], (after,))
            rel_mine, rel_state = adagrad_step(rel_mine, rel_state, g_rel, rel_sums, LEARN_REL, dim, swap, False)
            if round_idx < ent_size - 1:
                rel_other = lax.ppermute(rel_mine, "ent", core_swap)
            losses.append(jnp.where(part == 0, sums[0], sums[1]) / edge_count)

        ent_out = join_columns(part, ent_cols, ent_cols_peer).T
        rel_cols = flip_half(rel_mine, dim)
        quarter = rel_cols.shape[-1] // 2
        chip = lax.axis_index("ent") // 2
        piece = lax.ppermute(lax.dynamic_slice_in_dim(rel_cols, chip * quarter, quarter, axis=1), "data", swap)
        piece_other = lax.ppermute(piece, "ent", chip_swap)
        rel_peer = jnp.concatenate(
            [jnp.where(chip == 0, piece, piece_other), jnp.where(chip == 0, piece_other, piece)], axis=1)
        rel_all = join_columns(part, rel_cols, rel_peer)
        rel_other = lax.ppermute(rel_all, "ent", core_swap)
        rel_out = jnp.concatenate(
            [jnp.where(core == 0, rel_all, rel_other), jnp.where(core == 0, rel_other, rel_all)], axis=1).T
        return ent_out, state.reshape(-1), rel_out, jnp.stack(losses)[None, None, :]

    ent_spec = P(("sweep", "ent"), None)
    row_spec = P(("sweep", "ent"))
    rel_spec = P("sweep", None)
    edge_spec = P(("sweep", "ent"), "data", None, None)
    loss_spec = P(("sweep", "ent"), "data", None)
    return jax.shard_map(
        device_epoch, mesh=mesh,
        in_specs=(ent_spec, row_spec, rel_spec, edge_spec, edge_spec, edge_spec, edge_spec, edge_spec),
        out_specs=(ent_spec, row_spec, rel_spec, loss_spec),
        check_vma=False)
```

```python
import functools

import jax
import jax.numpy as jnp
from jax import lax
from jax.experimental import pallas as pl
from jax.experimental.pallas import tpu as pltpu
from jax.sharding import PartitionSpec as P


LEARN_ENT = 0.1
LEARN_REL = 0.05
ADA_EPS = 1e-6
LANES = 128
BLOCK = 256
WIDE_ROWS = 512
PIECES = 4
VMEM_CAP = 66_000_000


def pair_at(row):
    return pl.ds(pl.multiple_of(row, 2), 2)


def halves(ref):
    count = ref.shape[0] // 2
    return ref[pl.ds(0, count, stride=2), :], ref[pl.ds(1, count, stride=2), :]


def put_halves(ref, real, imag):
    count = ref.shape[0] // 2
    ref[pl.ds(0, count, stride=2), :] = real
    ref[pl.ds(1, count, stride=2), :] = imag


def split_kernel(width, part_ref, in_ref, out_ref, *bf_refs):
    second = part_ref[0] != 0
    lane = lax.broadcasted_iota(jnp.int32, (out_ref.shape[0] // 2, LANES), 1)

    def pick(start):
        last = in_ref.shape[0] - LANES
        shift = max(start - last, 0)
        rows = in_ref[pl.ds(start - shift, LANES), :].T
        if shift:
            rows = pltpu.roll(rows, LANES - shift, 1)
        return jnp.where(lane < width, rows, 0.0)

    real = jnp.where(second, pick(width), pick(0))
    imag = jnp.where(second, pick(3 * width), pick(2 * width))
    put_halves(out_ref, real, imag)
    for ref in bf_refs:
        ref[...] = out_ref[...].astype(jnp.bfloat16)


def split_columns(table, part, with_bf):
    rows, dim = table.shape
    pairs = pl.BlockSpec((2 * WIDE_ROWS, LANES), lambda b: (b, 0))
    kinds = [jnp.float32, jnp.bfloat16] if with_bf else [jnp.float32]
    return pl.pallas_call(
        functools.partial(split_kernel, dim // 4),
        grid=(pl.cdiv(rows, WIDE_ROWS),),
        in_specs=[pl.BlockSpec(memory_space=pltpu.SMEM), pl.BlockSpec((dim, WIDE_ROWS), lambda b: (0, b))],
        out_specs=[pairs] * len(kinds),
        out_shape=[jax.ShapeDtypeStruct((2 * rows, LANES), kind) for kind in kinds],
        compiler_params=pltpu.CompilerParams(dimension_semantics=("arbitrary",)),
        cost_estimate=pl.CostEstimate(flops=20_000_000, bytes_accessed=45_000_000, transcendentals=0),
        name="split_columns",
    )(part[None], table.T)


def flip_kernel(in_ref, out_ref):
    real, imag = halves(in_ref)
    width = out_ref.shape[0] // 2
    out_ref[pl.ds(0, width), :] = real.T[:width, :]
    out_ref[pl.ds(width, width), :] = imag.T[:width, :]


def flip_half(half, dim, start=0, rows=None):
    rows = half.shape[0] // 2 if rows is None else rows
    skip = start // WIDE_ROWS
    return pl.pallas_call(
        flip_kernel,
        grid=(pl.cdiv(rows, WIDE_ROWS),),
        in_specs=[pl.BlockSpec((2 * WIDE_ROWS, LANES), lambda b: (b + skip, 0))],
        out_specs=pl.BlockSpec((dim // 2, WIDE_ROWS), lambda b: (0, b)),
        out_shape=jax.ShapeDtypeStruct((dim // 2, rows), jnp.float32),
        compiler_params=pltpu.CompilerParams(dimension_semantics=("arbitrary",)),
        cost_estimate=pl.CostEstimate(flops=20_000_000, bytes_accessed=30_000_000, transcendentals=0),
        name="flip_half",
    )(half)


def query_kernel(core_ref, head_ref, rel_ref, ent_hbm, relm_hbm, relo_hbm, a_ref, r_ref, q_ref, ent_v, rel_v, sems):
    @pl.when(pl.program_id(0) == 0)
    def _():
        half = relm_hbm.shape[0]
        core = core_ref[0]
        mine = pl.ds(pl.multiple_of(core * half, 8), half)
        other = pl.ds(pl.multiple_of((1 - core) * half, 8), half)
        copies = [
            pltpu.make_async_copy(ent_hbm, ent_v, sems.at[0]),
            pltpu.make_async_copy(relm_hbm, rel_v.at[mine], sems.at[1]),
            pltpu.make_async_copy(relo_hbm, rel_v.at[other], sems.at[2]),
        ]
        for copy in copies:
            copy.start()
        for copy in copies:
            copy.wait()

    unroll = 32

    def some(step, carry):
        for sub in range(unroll):
            edge = step * unroll + sub
            a_ref[pair_at(2 * edge), :] = ent_v[pair_at(head_ref[0, 0, edge]), :]
            r_ref[pair_at(2 * edge), :] = rel_v[pair_at(rel_ref[0, 0, edge]), :]
        return carry

    lax.fori_loop(0, BLOCK // unroll, some, 0)
    a_re, a_im = halves(a_ref)
    r_re, r_im = halves(r_ref)
    q_ref[:, :LANES] = (a_re * r_re - a_im * r_im).astype(jnp.bfloat16)
    q_ref[:, LANES:] = (a_re * r_im + a_im * r_re).astype(jnp.bfloat16)


def tail_kernel(negs, tail_ref, neg_ref, a_ref, r_ref, tab_hbm, c_ref, p_ref, m_ref, tab_bf, tab_v, neg_v, sem):
    @pl.when(pl.program_id(0) == 0)
    def _():
        copy = pltpu.make_async_copy(tab_hbm, tab_bf, sem)
        copy.start()
        copy.wait()
        rows = 512

        def widen(step, carry):
            at = pl.ds(pl.multiple_of(step * rows, rows), rows)
            tab_v[at, :] = tab_bf[at, :].astype(jnp.float32)
            return carry

        lax.fori_loop(0, tab_v.shape[0] // rows, widen, 0)
        neg_v[...] = jnp.zeros_like(neg_v)
        small = 8

        def pick(step, carry):
            for sub in range(small):
                row = step * small + sub
                neg_v[pair_at(2 * row), :] = tab_v[pair_at(neg_ref[0, 0, row]), :]
            return carry

        lax.fori_loop(0, negs // small, pick, 0)
        m_re, m_im = halves(neg_v)
        m_ref[:, :LANES] = m_re.astype(jnp.bfloat16)
        m_ref[:, LANES:] = m_im.astype(jnp.bfloat16)

    unroll = 32

    def some(step, carry):
        for sub in range(unroll):
            edge = step * unroll + sub
            c_ref[pair_at(2 * edge), :] = tab_v[pair_at(tail_ref[0, 0, edge]), :]
        return carry

    lax.fori_loop(0, BLOCK // unroll, some, 0)
    a_re, a_im = halves(a_ref)
    r_re, r_im = halves(r_ref)
    c_re, c_im = halves(c_ref)
    prod = (a_re * r_re - a_im * r_im) * c_re + (a_re * r_im + a_im * r_re) * c_im
    p_ref[0] = jnp.sum(prod.T, axis=0, keepdims=True)


def column(row):
    return jnp.broadcast_to(row, (LANES, row.shape[-1])).T


def grad_kernel(
    last, negs,
    core_ref, head_ref, rel_ref, a_ref, r_ref, c_ref, qm_ref, qp_ref, pm_ref, pp_ref, w_ref, mm_ref, mp_ref,
    *rest,
):
    before, rest = rest[:2 * last], rest[2 * last:]
    outs, (t_ref, n_ref, loss_ref, acc_h, acc_r, blk_h, blk_r, neg_acc, sems) = rest[:2 + last], rest[2 + last:]
    block = pl.program_id(0)
    accs = (acc_h, acc_r)

    @pl.when(block == 0)
    def _():
        neg_acc[...] = jnp.zeros_like(neg_acc)
        loss_ref[...] = jnp.zeros_like(loss_ref)
        if last:
            copies = [pltpu.make_async_copy(src, acc, sems.at[slot]) for slot, (src, acc) in enumerate(zip(before, accs))]
            for copy in copies:
                copy.start()
            for copy in copies:
                copy.wait()
        else:
            for acc in accs:
                rows = max(size for size in range(8, 513, 8) if acc.shape[0] % size == 0)

                def clear(step, carry, acc=acc, rows=rows):
                    acc[pl.ds(pl.multiple_of(step * rows, rows), rows), :] = jnp.zeros((rows, LANES), jnp.float32)
                    return carry

                lax.fori_loop(0, acc.shape[0] // rows, clear, 0)

    a_re, a_im = halves(a_ref)
    r_re, r_im = halves(r_ref)
    c_re, c_im = halves(c_ref)
    q_re = a_re * r_re - a_im * r_im
    q_im = a_re * r_im + a_im * r_re
    q_bf = qm_ref[...]
    m_mine = mm_ref[...]
    nt = (((1,), (1,)), ((), ()))
    score = lax.dot_general(q_bf, m_mine, nt, preferred_element_type=jnp.float32)
    score = score + lax.dot_general(qp_ref[...], mp_ref[...], nt, preferred_element_type=jnp.float32)
    lane = lax.broadcasted_iota(jnp.int32, score.shape, 1)
    score = jnp.where(lane < negs, score, -jnp.inf)
    pos = column(pm_ref[0] + pp_ref[0])
    weight = column(w_ref[0])
    low, high = score[:, :LANES], score[:, LANES:]
    top = jnp.maximum(pos, jnp.max(jnp.maximum(low, high), axis=1, keepdims=True))
    pos_exp = jnp.exp(pos - top)
    low_exp, high_exp = jnp.exp(low - top), jnp.exp(high - top)
    norm = pos_exp + jnp.sum(low_exp + high_exp, axis=1, keepdims=True)
    loss_ref[...] += jnp.sum(weight * (top + jnp.log(norm) - pos), axis=0, keepdims=True)
    alpha = weight * (pos_exp / norm - 1.0)
    scale = weight / norm
    beta = jnp.concatenate([(scale * low_exp).astype(jnp.bfloat16), (scale * high_exp).astype(jnp.bfloat16)], axis=1)
    nn = (((1,), (0,)), ((), ()))
    mixed = lax.dot_general(beta, m_mine, nn, preferred_element_type=jnp.float32)
    tn = (((0,), (0,)), ((), ()))
    neg_acc[...] += lax.dot_general(beta, q_bf, tn, preferred_element_type=jnp.float32)
    d_re = alpha * c_re + mixed[:, :LANES]
    d_im = alpha * c_im + mixed[:, LANES:]
    put_halves(t_ref, alpha * q_re, alpha * q_im)
    put_halves(blk_h, d_re * r_re + d_im * r_im, d_im * r_re - d_re * r_im)
    put_halves(blk_r, d_re * a_re + d_im * a_im, d_im * a_re - d_re * a_im)

    unroll = 16

    def some(step, carry):
        for sub in range(unroll):
            edge = step * unroll + sub
            here = pair_at(2 * edge)
            at_h, at_r = (pair_at(ref[0, 0, edge]) for ref in (head_ref, rel_ref))
            acc_h[at_h, :] = acc_h[at_h, :] + blk_h[here, :]
            acc_r[at_r, :] = acc_r[at_r, :] + blk_r[here, :]
        return carry

    lax.fori_loop(0, BLOCK // unroll, some, 0)

    @pl.when(block == pl.num_programs(0) - 1)
    def _():
        put_halves(n_ref, neg_acc[:, :LANES], neg_acc[:, LANES:])
        sources = list(accs)
        if last:
            half = acc_r.shape[0] // 2
            core = core_ref[0]
            sources[1:] = [acc_r.at[pl.ds(pl.multiple_of(at * half, 8), half)] for at in (core, 1 - core)]
        copies = [pltpu.make_async_copy(src, out, sems.at[slot]) for slot, (src, out) in enumerate(zip(sources, outs))]
        for copy in copies:
            copy.start()
        for copy in copies:
            copy.wait()


def smem_block(width):
    return pl.BlockSpec((1, 1, width), lambda b: (b, 0, 0), memory_space=pltpu.SMEM)


PAIRS = pl.BlockSpec((2 * BLOCK, LANES), lambda b: (b, 0))
WIDE = pl.BlockSpec((BLOCK, 2 * LANES), lambda b: (b, 0))
ROW = pl.BlockSpec((1, 1, BLOCK), lambda b: (b, 0, 0))
NEGS = pl.BlockSpec((2 * LANES, 2 * LANES), lambda b: (0, 0))
ANYWHERE = pl.BlockSpec(memory_space=pl.ANY)
SCALARS = pl.BlockSpec(memory_space=pltpu.SMEM)
PARAMS = dict(dimension_semantics=("arbitrary",), vmem_limit_bytes=VMEM_CAP)


def query_rows(core, ent, rel_mine, rel_other, head_ids, rel_ids):
    blocks = head_ids.shape[0]
    edges = blocks * BLOCK
    return pl.pallas_call(
        query_kernel,
        grid=(blocks,),
        in_specs=[SCALARS, smem_block(BLOCK), smem_block(BLOCK), ANYWHERE, ANYWHERE, ANYWHERE],
        out_specs=[PAIRS, PAIRS, WIDE],
        out_shape=[
            jax.ShapeDtypeStruct((2 * edges, LANES), jnp.float32),
            jax.ShapeDtypeStruct((2 * edges, LANES), jnp.float32),
            jax.ShapeDtypeStruct((edges, 2 * LANES), jnp.bfloat16),
        ],
        scratch_shapes=[
            pltpu.VMEM(ent.shape, jnp.float32),
            pltpu.VMEM((2 * rel_mine.shape[0], LANES), jnp.float32),
            pltpu.SemaphoreType.DMA((3,)),
        ],
        compiler_params=pltpu.CompilerParams(**PARAMS),
        cost_estimate=pl.CostEstimate(flops=100_000_000, bytes_accessed=80_000_000, transcendentals=0),
        name="query_rows",
    )(core, head_ids, rel_ids, ent, rel_mine, rel_other)


def tail_rows(table, tail_ids, neg_ids, a_rows, r_rows):
    blocks = tail_ids.shape[0]
    edges = blocks * BLOCK
    negs = neg_ids.shape[-1]
    return pl.pallas_call(
        functools.partial(tail_kernel, negs),
        grid=(blocks,),
        in_specs=[smem_block(BLOCK), SCALARS, PAIRS, PAIRS, ANYWHERE],
        out_specs=[PAIRS, ROW, NEGS],
        out_shape=[
            jax.ShapeDtypeStruct((2 * edges, LANES), jnp.float32),
            jax.ShapeDtypeStruct((blocks, 1, BLOCK), jnp.float32),
            jax.ShapeDtypeStruct((2 * LANES, 2 * LANES), jnp.bfloat16),
        ],
        scratch_shapes=[
            pltpu.VMEM(table.shape, jnp.bfloat16),
            pltpu.VMEM(table.shape, jnp.float32),
            pltpu.VMEM((4 * LANES, LANES), jnp.float32),
            pltpu.SemaphoreType.DMA,
        ],
        compiler_params=pltpu.CompilerParams(**PARAMS),
        cost_estimate=pl.CostEstimate(flops=100_000_000, bytes_accessed=60_000_000, transcendentals=0),
        name="tail_rows",
    )(tail_ids, neg_ids, a_rows, r_rows, table)


def bucket_grads(core, ids, negs, rows, queries, scores, weight, negatives, before, ent_shape, rel_shape):
    blocks = ids[0].shape[0]
    last = before is not None
    before = before or ()
    half_shape = (rel_shape[0] // 2, LANES)
    shapes = [ent_shape] + ([half_shape, half_shape] if last else [rel_shape])
    neg_pairs = (4 * LANES, LANES)
    flat = lambda b: (0, 0)
    return pl.pallas_call(
        functools.partial(grad_kernel, int(last), negs),
        grid=(blocks,),
        in_specs=[SCALARS] + [smem_block(BLOCK)] * 2 + [PAIRS] * 3 + [WIDE] * 2 + [ROW] * 3 + [NEGS] * 2
        + [ANYWHERE] * len(before),
        out_specs=[ANYWHERE] * len(shapes) + [PAIRS, pl.BlockSpec(neg_pairs, flat), pl.BlockSpec((1, LANES), flat)],
        out_shape=[
            jax.ShapeDtypeStruct(shape, jnp.float32)
            for shape in shapes + [(2 * blocks * BLOCK, LANES), neg_pairs, (1, LANES)]
        ],
        scratch_shapes=[
            pltpu.VMEM(ent_shape, jnp.float32),
            pltpu.VMEM(rel_shape, jnp.float32),
            pltpu.VMEM((2 * BLOCK, LANES), jnp.float32),
            pltpu.VMEM((2 * BLOCK, LANES), jnp.float32),
            pltpu.VMEM((2 * LANES, 2 * LANES), jnp.float32),
            pltpu.SemaphoreType.DMA((3,)),
        ],
        compiler_params=pltpu.CompilerParams(**PARAMS),
        cost_estimate=pl.CostEstimate(flops=300_000_000, bytes_accessed=200_000_000, transcendentals=2_000_000),
        name="bucket_grads",
    )(core, *ids, *rows, *queries, *scores, weight, *negatives, *before)


def add_kernel(negs, tail_ref, neg_ref, rows_ref, n_ref, base_hbm, g_hbm, *rest):
    sum_refs, (acc, sem) = rest[:-2], rest[-2:]
    block = pl.program_id(0)

    @pl.when(block == 0)
    def _():
        copy = pltpu.make_async_copy(base_hbm, acc, sem)
        copy.start()
        copy.wait()
        small = 8

        def more(step, carry):
            for sub in range(small):
                row = step * small + sub
                at = pair_at(neg_ref[0, 0, row])
                acc[at, :] = acc[at, :] + n_ref[pair_at(2 * row), :]
            return carry

        lax.fori_loop(0, negs // small, more, 0)

    unroll = 16

    def some(step, carry):
        for sub in range(unroll):
            edge = step * unroll + sub
            at = pair_at(tail_ref[0, 0, edge])
            acc[at, :] = acc[at, :] + rows_ref[pair_at(2 * edge), :]
        return carry

    lax.fori_loop(0, BLOCK // unroll, some, 0)

    @pl.when(block == pl.num_programs(0) - 1)
    def _():
        copy = pltpu.make_async_copy(acc, g_hbm, sem)
        copy.start()
        for sum_ref in sum_refs:
            width = sum_ref.shape[-1]

            def square(step, carry):
                start = pl.multiple_of(step * 2 * width, 2 * width)
                real = acc[pl.ds(start, width, stride=2), :]
                imag = acc[pl.ds(start + 1, width, stride=2), :]
                sum_ref[step] = jnp.sum((real * real + imag * imag).T, axis=0, keepdims=True)
                return carry

            lax.fori_loop(0, sum_ref.shape[0], square, 0)
        copy.wait()


def add_rows(base, tail_ids, neg_ids, rows, neg_rows, sum_shape):
    blocks = tail_ids.shape[0]
    sums = [] if sum_shape is None else [sum_shape]
    return pl.pallas_call(
        functools.partial(add_kernel, neg_ids.shape[-1]),
        grid=(blocks,),
        in_specs=[smem_block(BLOCK), SCALARS, PAIRS, pl.BlockSpec(neg_rows.shape, lambda b: (0, 0)), ANYWHERE],
        out_specs=[ANYWHERE] + [pl.BlockSpec(shape, lambda b: (0, 0, 0)) for shape in sums],
        out_shape=[jax.ShapeDtypeStruct(shape, jnp.float32) for shape in [base.shape] + sums],
        scratch_shapes=[pltpu.VMEM(base.shape, jnp.float32), pltpu.SemaphoreType.DMA],
        compiler_params=pltpu.CompilerParams(**PARAMS),
        cost_estimate=pl.CostEstimate(flops=100_000_000, bytes_accessed=100_000_000, transcendentals=0),
        name="add_rows",
    )(tail_ids, neg_ids, rows, neg_rows, base)


def square_kernel(one_ref, two_ref, *rest):
    g_ref, sum_ref = rest[-2:]
    g_ref[...] = one_ref[...] + two_ref[...]
    real, imag = halves(g_ref)
    sum_ref[0] = jnp.sum((real * real + imag * imag).T, axis=0, keepdims=True)


def step_kernel(rate, dim, par_ref, g_ref, state_ref, sm_ref, sp_ref, out_ref, new_ref, *bf_refs):
    state = state_ref[0] + (sm_ref[0] + sp_ref[0]) / dim
    new_ref[0] = state
    scale = column(rate / jnp.sqrt(state + ADA_EPS))
    p_re, p_im = halves(par_ref)
    g_re, g_im = halves(g_ref)
    put_halves(out_ref, p_re - g_re * scale, p_im - g_im * scale)
    for ref in bf_refs:
        ref[...] = out_ref[...].astype(jnp.bfloat16)


PAIR_ROWS = pl.BlockSpec((2 * WIDE_ROWS, LANES), lambda b: (b, 0))
WIDE_ROW = pl.BlockSpec((1, 1, WIDE_ROWS), lambda b: (b, 0, 0))


def square_sums(one, two, blocks, after):
    return pl.pallas_call(
        square_kernel,
        grid=(blocks,),
        in_specs=[PAIR_ROWS, PAIR_ROWS] + [ANYWHERE] * len(after),
        out_specs=[PAIR_ROWS, WIDE_ROW],
        out_shape=[
            jax.ShapeDtypeStruct(one.shape, jnp.float32),
            jax.ShapeDtypeStruct((blocks, 1, WIDE_ROWS), jnp.float32),
        ],
        compiler_params=pltpu.CompilerParams(dimension_semantics=("arbitrary",)),
        cost_estimate=pl.CostEstimate(flops=4 * one.size, bytes_accessed=12 * one.size, transcendentals=0),
        name="square_sums",
    )(one, two, *after)


def adagrad_step(param, state, grad, sums, rate, dim, swap, with_bf):
    sums_peer = lax.ppermute(sums, "data", swap)
    kinds = [jnp.float32, jnp.bfloat16] if with_bf else [jnp.float32]
    wide = [jax.ShapeDtypeStruct(param.shape, kind) for kind in kinds]
    return pl.pallas_call(
        functools.partial(step_kernel, rate, dim),
        grid=(state.shape[0],),
        in_specs=[PAIR_ROWS, PAIR_ROWS, WIDE_ROW, WIDE_ROW, WIDE_ROW],
        out_specs=[PAIR_ROWS, WIDE_ROW] + [PAIR_ROWS] * (len(kinds) - 1),
        out_shape=[wide[0], jax.ShapeDtypeStruct(state.shape, jnp.float32)] + wide[1:],
        compiler_params=pltpu.CompilerParams(dimension_semantics=("arbitrary",)),
        cost_estimate=pl.CostEstimate(flops=4 * param.size, bytes_accessed=12 * param.size, transcendentals=0),
        name="adagrad_step",
    )(param, grad, state, sums, sums_peer)


def join_kernel(part_ref, mine_ref, peer_ref, *rest):
    out_ref = rest[-1]
    second = part_ref[0] != 0
    width = mine_ref.shape[0] // 2
    for side in range(2):
        mine, peer = (ref[pl.ds(side * width, width), :] for ref in (mine_ref, peer_ref))
        out_ref[pl.ds(2 * side * width, width), :] = jnp.where(second, peer, mine)
        out_ref[pl.ds((2 * side + 1) * width, width), :] = jnp.where(second, mine, peer)


def join_columns(part, mine, peer, start=0, total=None, whole=()):
    width, rows = mine.shape
    skip = start // WIDE_ROWS
    half = pl.BlockSpec((width, WIDE_ROWS), lambda b: (0, b))
    return pl.pallas_call(
        join_kernel,
        grid=(pl.cdiv(rows, WIDE_ROWS),),
        in_specs=[SCALARS, half, half] + [ANYWHERE] * len(whole),
        out_specs=pl.BlockSpec((2 * width, WIDE_ROWS), lambda b: (0, b + skip)),
        out_shape=jax.ShapeDtypeStruct((2 * width, total or rows), jnp.float32),
        input_output_aliases={3: 0} if whole else {},
        compiler_params=pltpu.CompilerParams(dimension_semantics=("arbitrary",)),
        cost_estimate=pl.CostEstimate(flops=mine.size, bytes_accessed=16 * mine.size, transcendentals=0),
        name="join_columns",
    )(part[None], mine, peer, *whole)


def solution(mesh):
    ent_size = mesh.shape["ent"]
    data_size = mesh.shape["data"]
    swap = [(src, data_size - 1 - src) for src in range(data_size)]
    core_swap = [(src, src ^ 1) for src in range(ent_size)]
    chip_swap = [(src, src ^ 2) for src in range(ent_size)]

    def device_epoch(ent_table, ada_state, rel_table, head_idx, tail_idx, rel_idx, edge_mask, neg_idx):
        ent_rows, dim = ent_table.shape
        rel_rows = rel_table.shape[0]
        edge_count = head_idx.shape[-1]
        negs = neg_idx.shape[-1]
        part = lax.axis_index("data")
        core = lax.rem(lax.axis_index("ent"), 2)
        core_at = core[None]
        ent, table = split_columns(ent_table, part, True)
        rel = split_columns(rel_table, part, False)[0]
        ent_shape, rel_shape = ent.shape, rel.shape
        rel_mine = lax.dynamic_slice_in_dim(rel, core * rel_rows, rel_rows, axis=0)
        rel_other = lax.dynamic_slice_in_dim(rel, (1 - core) * rel_rows, rel_rows, axis=0)
        state = ada_state.reshape(-1, 1, WIDE_ROWS)
        rel_state = jnp.zeros((pl.cdiv(rel_rows // 2, WIDE_ROWS), 1, WIDE_ROWS), jnp.float32)

        local = jnp.concatenate(
            [2 * head_idx[0, 0], 2 * tail_idx[0, 0], 2 * rel_idx[0, 0], edge_mask[0, 0], 2 * neg_idx[0, 0]], axis=1)
        both = lax.all_gather(local, "data")
        blocks = edge_count // BLOCK

        def field(slot, bucket, round_idx):
            return both[bucket, round_idx, slot * edge_count:(slot + 1) * edge_count].reshape(blocks, 1, BLOCK)

        def owned(round_idx):
            mine = jnp.concatenate(
                [both[:, round_idx, edge_count:2 * edge_count], both[:, round_idx, 4 * edge_count:]], axis=1)
            if round_idx:
                mine = lax.ppermute(mine, "ent", [(src, (src + round_idx) % ent_size) for src in range(ent_size)])
            return [
                (mine[bucket, :edge_count].reshape(blocks, 1, BLOCK), mine[bucket, edge_count:].reshape(1, 1, negs))
                for bucket in range(data_size)
            ]

        losses = []
        for round_idx in range(ent_size):
            if round_idx:
                fetch = [((dest + round_idx) % ent_size, dest) for dest in range(ent_size)]
                table = lax.ppermute(table, "ent", fetch)
            ids = [[field(slot, bucket, round_idx) for slot in range(3)] for bucket in range(data_size)]
            asked = []
            for bucket in range(data_size):
                asked.append(query_rows(core_at, ent, rel_mine, rel_other, ids[bucket][0], ids[bucket][2]))
            back = [(src, (src + round_idx) % ent_size) for src in range(ent_size)]
            targets = owned(round_idx)
            before = None
            sums, returned = [], []
            for bucket in range(data_size):
                a_rows, r_rows, q_mine = asked[bucket]
                q_peer = lax.ppermute(q_mine, "data", swap)
                neg_ids = both[bucket, round_idx, 4 * edge_count:].reshape(1, 1, negs)
                c_rows, p_mine, m_mine = tail_rows(table, ids[bucket][1], neg_ids, a_rows, r_rows)
                m_peer = lax.ppermute(m_mine, "data", swap)
                p_peer = lax.ppermute(p_mine, "data", swap)
                *before, t_rows, n_rows, loss = bucket_grads(
                    core_at, (ids[bucket][0], ids[bucket][2]), negs, (a_rows, r_rows, c_rows), (q_mine, q_peer),
                    (p_mine, p_peer), field(3, bucket, round_idx).astype(jnp.float32), (m_mine, m_peer), before,
                    ent_shape, rel_shape)
                sums.append(loss[0, 0])
                if round_idx:
                    t_rows = lax.ppermute(t_rows, "ent", back)
                    n_rows = lax.ppermute(n_rows, "ent", back)
                returned.append((t_rows, n_rows))
            g_ent, keep, give = before
            chip_sum = keep + lax.ppermute(give, "ent", core_swap)
            chip_other = lax.ppermute(chip_sum, "ent", chip_swap)
            for bucket in range(data_size):
                shape = state.shape if bucket == data_size - 1 else None
                g_ent, *ent_sums = add_rows(g_ent, *targets[bucket], *returned[bucket], shape)
            ent, state, table = adagrad_step(ent, state, g_ent, ent_sums[0], LEARN_ENT, dim, swap, True)
            after = state
            if round_idx == ent_size - 1:
                size = ent_rows // PIECES
                ent_cols = [flip_half(ent, dim, piece * size, size) for piece in range(PIECES)]
                after = ent_cols[0]
                ent_peer = []
                for piece in range(PIECES):
                    ent_peer.append(lax.ppermute(ent_cols[piece], "data", swap))
            g_rel, rel_sums = square_sums(chip_sum, chip_other, rel_state.shape[0], (after,))
            rel_mine, rel_state = adagrad_step(rel_mine, rel_state, g_rel, rel_sums, LEARN_REL, dim, swap, False)
            if round_idx < ent_size - 1:
                rel_other = lax.ppermute(rel_mine, "ent", core_swap)
            losses.append(jnp.where(part == 0, sums[0], sums[1]) / edge_count)

        ent_out = ()
        for piece in range(PIECES):
            ent_out = (join_columns(part, ent_cols[piece], ent_peer[piece], piece * size, ent_rows, ent_out),)
        ent_out = ent_out[0].T
        rel_cols = flip_half(rel_mine, dim)
        quarter = rel_cols.shape[-1] // 2
        chip = lax.axis_index("ent") // 2
        piece = lax.ppermute(lax.dynamic_slice_in_dim(rel_cols, chip * quarter, quarter, axis=1), "data", swap)
        piece_other = lax.ppermute(piece, "ent", chip_swap)
        rel_peer = jnp.concatenate(
            [jnp.where(chip == 0, piece, piece_other), jnp.where(chip == 0, piece_other, piece)], axis=1)
        rel_all = join_columns(part, rel_cols, rel_peer)
        rel_other = lax.ppermute(rel_all, "ent", core_swap)
        rel_out = jnp.concatenate(
            [jnp.where(core == 0, rel_all, rel_other), jnp.where(core == 0, rel_other, rel_all)], axis=1).T
        return ent_out, state.reshape(-1), rel_out, jnp.stack(losses)[None, None, :]

    ent_spec = P(("sweep", "ent"), None)
    row_spec = P(("sweep", "ent"))
    rel_spec = P("sweep", None)
    edge_spec = P(("sweep", "ent"), "data", None, None)
    loss_spec = P(("sweep", "ent"), "data", None)
    return jax.shard_map(
        device_epoch, mesh=mesh,
        in_specs=(ent_spec, row_spec, rel_spec, edge_spec, edge_spec, edge_spec, edge_spec, edge_spec),
        out_specs=(ent_spec, row_spec, rel_spec, loss_spec),
        check_vma=False)
```

```python
import functools

import jax
import jax.numpy as jnp
from jax import lax
from jax.experimental import pallas as pl
from jax.experimental.pallas import tpu as pltpu
from jax.sharding import PartitionSpec as P


LEARN_ENT = 0.1
LEARN_REL = 0.05
ADA_EPS = 1e-6
LANES = 128
BLOCK = 256
WIDE_ROWS = 512
PIECES = 4
VMEM_CAP = 66_000_000


def pair_at(row):
    return pl.ds(pl.multiple_of(row, 2), 2)


def halves(ref):
    count = ref.shape[0] // 2
    return ref[pl.ds(0, count, stride=2), :], ref[pl.ds(1, count, stride=2), :]


def put_halves(ref, real, imag):
    count = ref.shape[0] // 2
    ref[pl.ds(0, count, stride=2), :] = real
    ref[pl.ds(1, count, stride=2), :] = imag


def split_kernel(width, part_ref, in_ref, out_ref, *bf_refs):
    second = part_ref[0] != 0
    lane = lax.broadcasted_iota(jnp.int32, (out_ref.shape[0] // 2, LANES), 1)

    def pick(start):
        last = in_ref.shape[0] - LANES
        shift = max(start - last, 0)
        rows = in_ref[pl.ds(start - shift, LANES), :].T
        if shift:
            rows = pltpu.roll(rows, LANES - shift, 1)
        return jnp.where(lane < width, rows, 0.0)

    real = jnp.where(second, pick(width), pick(0))
    imag = jnp.where(second, pick(3 * width), pick(2 * width))
    put_halves(out_ref, real, imag)
    for ref in bf_refs:
        ref[...] = out_ref[...].astype(jnp.bfloat16)


def split_columns(table, part, with_bf):
    rows, dim = table.shape
    pairs = pl.BlockSpec((2 * WIDE_ROWS, LANES), lambda b: (b, 0))
    kinds = [jnp.float32, jnp.bfloat16] if with_bf else [jnp.float32]
    return pl.pallas_call(
        functools.partial(split_kernel, dim // 4),
        grid=(pl.cdiv(rows, WIDE_ROWS),),
        in_specs=[pl.BlockSpec(memory_space=pltpu.SMEM), pl.BlockSpec((dim, WIDE_ROWS), lambda b: (0, b))],
        out_specs=[pairs] * len(kinds),
        out_shape=[jax.ShapeDtypeStruct((2 * rows, LANES), kind) for kind in kinds],
        compiler_params=pltpu.CompilerParams(dimension_semantics=("arbitrary",)),
        cost_estimate=pl.CostEstimate(flops=20_000_000, bytes_accessed=45_000_000, transcendentals=0),
        name="split_columns",
    )(part[None], table.T)


def flip_kernel(in_ref, out_ref):
    real, imag = halves(in_ref)
    width = out_ref.shape[0] // 2
    out_ref[pl.ds(0, width), :] = real.T[:width, :]
    out_ref[pl.ds(width, width), :] = imag.T[:width, :]


def flip_half(half, dim, start=0, rows=None):
    rows = half.shape[0] // 2 if rows is None else rows
    skip = start // WIDE_ROWS
    return pl.pallas_call(
        flip_kernel,
        grid=(pl.cdiv(rows, WIDE_ROWS),),
        in_specs=[pl.BlockSpec((2 * WIDE_ROWS, LANES), lambda b: (b + skip, 0))],
        out_specs=pl.BlockSpec((dim // 2, WIDE_ROWS), lambda b: (0, b)),
        out_shape=jax.ShapeDtypeStruct((dim // 2, rows), jnp.float32),
        compiler_params=pltpu.CompilerParams(dimension_semantics=("arbitrary",)),
        cost_estimate=pl.CostEstimate(flops=20_000_000, bytes_accessed=30_000_000, transcendentals=0),
        name="flip_half",
    )(half)


def query_kernel(core_ref, head_ref, rel_ref, ent_hbm, relm_hbm, relo_hbm, a_ref, r_ref, q_ref, ent_v, rel_v, sems):
    @pl.when(pl.program_id(0) == 0)
    def _():
        half = relm_hbm.shape[0]
        core = core_ref[0]
        mine = pl.ds(pl.multiple_of(core * half, 8), half)
        other = pl.ds(pl.multiple_of((1 - core) * half, 8), half)
        copies = [
            pltpu.make_async_copy(ent_hbm, ent_v, sems.at[0]),
            pltpu.make_async_copy(relm_hbm, rel_v.at[mine], sems.at[1]),
            pltpu.make_async_copy(relo_hbm, rel_v.at[other], sems.at[2]),
        ]
        for copy in copies:
            copy.start()
        for copy in copies:
            copy.wait()

    unroll = 32

    def some(step, carry):
        for sub in range(unroll):
            edge = step * unroll + sub
            a_ref[pair_at(2 * edge), :] = ent_v[pair_at(head_ref[0, 0, edge]), :]
            r_ref[pair_at(2 * edge), :] = rel_v[pair_at(rel_ref[0, 0, edge]), :]
        return carry

    lax.fori_loop(0, BLOCK // unroll, some, 0)
    a_re, a_im = halves(a_ref)
    r_re, r_im = halves(r_ref)
    q_ref[:, :LANES] = (a_re * r_re - a_im * r_im).astype(jnp.bfloat16)
    q_ref[:, LANES:] = (a_re * r_im + a_im * r_re).astype(jnp.bfloat16)


def tail_kernel(negs, tail_ref, neg_ref, a_ref, r_ref, tab_hbm, c_ref, p_ref, m_ref, tab_bf, tab_v, neg_v, sem):
    @pl.when(pl.program_id(0) == 0)
    def _():
        copy = pltpu.make_async_copy(tab_hbm, tab_bf, sem)
        copy.start()
        copy.wait()
        rows = 512

        def widen(step, carry):
            at = pl.ds(pl.multiple_of(step * rows, rows), rows)
            tab_v[at, :] = tab_bf[at, :].astype(jnp.float32)
            return carry

        lax.fori_loop(0, tab_v.shape[0] // rows, widen, 0)
        neg_v[...] = jnp.zeros_like(neg_v)
        small = 8

        def pick(step, carry):
            for sub in range(small):
                row = step * small + sub
                neg_v[pair_at(2 * row), :] = tab_v[pair_at(neg_ref[0, 0, row]), :]
            return carry

        lax.fori_loop(0, negs // small, pick, 0)
        m_re, m_im = halves(neg_v)
        m_ref[:, :LANES] = m_re.astype(jnp.bfloat16)
        m_ref[:, LANES:] = m_im.astype(jnp.bfloat16)

    unroll = 32

    def some(step, carry):
        for sub in range(unroll):
            edge = step * unroll + sub
            c_ref[pair_at(2 * edge), :] = tab_v[pair_at(tail_ref[0, 0, edge]), :]
        return carry

    lax.fori_loop(0, BLOCK // unroll, some, 0)
    a_re, a_im = halves(a_ref)
    r_re, r_im = halves(r_ref)
    c_re, c_im = halves(c_ref)
    prod = (a_re * r_re - a_im * r_im) * c_re + (a_re * r_im + a_im * r_re) * c_im
    p_ref[0] = jnp.sum(prod.T, axis=0, keepdims=True)


def column(row):
    return jnp.broadcast_to(row, (LANES, row.shape[-1])).T


def grad_kernel(
    last, negs,
    core_ref, head_ref, rel_ref, a_ref, r_ref, c_ref, qm_ref, qp_ref, pm_ref, pp_ref, w_ref, mm_ref, mp_ref,
    *rest,
):
    before, rest = rest[:2 * last], rest[2 * last:]
    outs, (t_ref, n_ref, loss_ref, acc_h, acc_r, blk_h, blk_r, neg_acc, sems) = rest[:2 + last], rest[2 + last:]
    block = pl.program_id(0)
    accs = (acc_h, acc_r)

    @pl.when(block == 0)
    def _():
        neg_acc[...] = jnp.zeros_like(neg_acc)
        loss_ref[...] = jnp.zeros_like(loss_ref)
        if last:
            copies = [pltpu.make_async_copy(src, acc, sems.at[slot]) for slot, (src, acc) in enumerate(zip(before, accs))]
            for copy in copies:
                copy.start()
            for copy in copies:
                copy.wait()
        else:
            for acc in accs:
                rows = max(size for size in range(8, 513, 8) if acc.shape[0] % size == 0)

                def clear(step, carry, acc=acc, rows=rows):
                    acc[pl.ds(pl.multiple_of(step * rows, rows), rows), :] = jnp.zeros((rows, LANES), jnp.float32)
                    return carry

                lax.fori_loop(0, acc.shape[0] // rows, clear, 0)

    a_re, a_im = halves(a_ref)
    r_re, r_im = halves(r_ref)
    c_re, c_im = halves(c_ref)
    q_re = a_re * r_re - a_im * r_im
    q_im = a_re * r_im + a_im * r_re
    q_bf = qm_ref[...]
    m_mine = mm_ref[...]
    nt = (((1,), (1,)), ((), ()))
    score = lax.dot_general(q_bf, m_mine, nt, preferred_element_type=jnp.float32)
    score = score + lax.dot_general(qp_ref[...], mp_ref[...], nt, preferred_element_type=jnp.float32)
    lane = lax.broadcasted_iota(jnp.int32, score.shape, 1)
    score = jnp.where(lane < negs, score, -jnp.inf)
    pos = column(pm_ref[0] + pp_ref[0])
    weight = column(w_ref[0])
    low, high = score[:, :LANES], score[:, LANES:]
    top = jnp.maximum(pos, jnp.max(jnp.maximum(low, high), axis=1, keepdims=True))
    pos_exp = jnp.exp(pos - top)
    low_exp, high_exp = jnp.exp(low - top), jnp.exp(high - top)
    norm = pos_exp + jnp.sum(low_exp + high_exp, axis=1, keepdims=True)
    loss_ref[...] += jnp.sum(weight * (top + jnp.log(norm) - pos), axis=0, keepdims=True)
    alpha = weight * (pos_exp / norm - 1.0)
    scale = weight / norm
    beta = jnp.concatenate([(scale * low_exp).astype(jnp.bfloat16), (scale * high_exp).astype(jnp.bfloat16)], axis=1)
    nn = (((1,), (0,)), ((), ()))
    mixed = lax.dot_general(beta, m_mine, nn, preferred_element_type=jnp.float32)
    tn = (((0,), (0,)), ((), ()))
    neg_acc[...] += lax.dot_general(beta, q_bf, tn, preferred_element_type=jnp.float32)
    d_re = alpha * c_re + mixed[:, :LANES]
    d_im = alpha * c_im + mixed[:, LANES:]
    put_halves(t_ref, alpha * q_re, alpha * q_im)
    put_halves(blk_h, d_re * r_re + d_im * r_im, d_im * r_re - d_re * r_im)
    put_halves(blk_r, d_re * a_re + d_im * a_im, d_im * a_re - d_re * a_im)

    unroll = 16

    def some(step, carry):
        for sub in range(unroll):
            edge = step * unroll + sub
            here = pair_at(2 * edge)
            at_h, at_r = (pair_at(ref[0, 0, edge]) for ref in (head_ref, rel_ref))
            acc_h[at_h, :] = acc_h[at_h, :] + blk_h[here, :]
            acc_r[at_r, :] = acc_r[at_r, :] + blk_r[here, :]
        return carry

    lax.fori_loop(0, BLOCK // unroll, some, 0)

    @pl.when(block == pl.num_programs(0) - 1)
    def _():
        put_halves(n_ref, neg_acc[:, :LANES], neg_acc[:, LANES:])
        sources = list(accs)
        if last:
            half = acc_r.shape[0] // 2
            core = core_ref[0]
            sources[1:] = [acc_r.at[pl.ds(pl.multiple_of(at * half, 8), half)] for at in (core, 1 - core)]
        copies = [pltpu.make_async_copy(src, out, sems.at[slot]) for slot, (src, out) in enumerate(zip(sources, outs))]
        for copy in copies:
            copy.start()
        for copy in copies:
            copy.wait()


def smem_block(width):
    return pl.BlockSpec((1, 1, width), lambda b: (b, 0, 0), memory_space=pltpu.SMEM)


PAIRS = pl.BlockSpec((2 * BLOCK, LANES), lambda b: (b, 0))
WIDE = pl.BlockSpec((BLOCK, 2 * LANES), lambda b: (b, 0))
ROW = pl.BlockSpec((1, 1, BLOCK), lambda b: (b, 0, 0))
NEGS = pl.BlockSpec((2 * LANES, 2 * LANES), lambda b: (0, 0))
ANYWHERE = pl.BlockSpec(memory_space=pl.ANY)
SCALARS = pl.BlockSpec(memory_space=pltpu.SMEM)
PARAMS = dict(dimension_semantics=("arbitrary",), vmem_limit_bytes=VMEM_CAP)


def query_rows(core, ent, rel_mine, rel_other, head_ids, rel_ids):
    blocks = head_ids.shape[0]
    edges = blocks * BLOCK
    return pl.pallas_call(
        query_kernel,
        grid=(blocks,),
        in_specs=[SCALARS, smem_block(BLOCK), smem_block(BLOCK), ANYWHERE, ANYWHERE, ANYWHERE],
        out_specs=[PAIRS, PAIRS, WIDE],
        out_shape=[
            jax.ShapeDtypeStruct((2 * edges, LANES), jnp.float32),
            jax.ShapeDtypeStruct((2 * edges, LANES), jnp.float32),
            jax.ShapeDtypeStruct((edges, 2 * LANES), jnp.bfloat16),
        ],
        scratch_shapes=[
            pltpu.VMEM(ent.shape, jnp.float32),
            pltpu.VMEM((2 * rel_mine.shape[0], LANES), jnp.float32),
            pltpu.SemaphoreType.DMA((3,)),
        ],
        compiler_params=pltpu.CompilerParams(**PARAMS),
        cost_estimate=pl.CostEstimate(flops=100_000_000, bytes_accessed=80_000_000, transcendentals=0),
        name="query_rows",
    )(core, head_ids, rel_ids, ent, rel_mine, rel_other)


def tail_rows(table, tail_ids, neg_ids, a_rows, r_rows):
    blocks = tail_ids.shape[0]
    edges = blocks * BLOCK
    negs = neg_ids.shape[-1]
    return pl.pallas_call(
        functools.partial(tail_kernel, negs),
        grid=(blocks,),
        in_specs=[smem_block(BLOCK), SCALARS, PAIRS, PAIRS, ANYWHERE],
        out_specs=[PAIRS, ROW, NEGS],
        out_shape=[
            jax.ShapeDtypeStruct((2 * edges, LANES), jnp.float32),
            jax.ShapeDtypeStruct((blocks, 1, BLOCK), jnp.float32),
            jax.ShapeDtypeStruct((2 * LANES, 2 * LANES), jnp.bfloat16),
        ],
        scratch_shapes=[
            pltpu.VMEM(table.shape, jnp.bfloat16),
            pltpu.VMEM(table.shape, jnp.float32),
            pltpu.VMEM((4 * LANES, LANES), jnp.float32),
            pltpu.SemaphoreType.DMA,
        ],
        compiler_params=pltpu.CompilerParams(**PARAMS),
        cost_estimate=pl.CostEstimate(flops=100_000_000, bytes_accessed=60_000_000, transcendentals=0),
        name="tail_rows",
    )(tail_ids, neg_ids, a_rows, r_rows, table)


def bucket_grads(core, ids, negs, rows, queries, scores, weight, negatives, before, ent_shape, rel_shape):
    blocks = ids[0].shape[0]
    last = before is not None
    before = before or ()
    half_shape = (rel_shape[0] // 2, LANES)
    shapes = [ent_shape] + ([half_shape, half_shape] if last else [rel_shape])
    neg_pairs = (4 * LANES, LANES)
    flat = lambda b: (0, 0)
    return pl.pallas_call(
        functools.partial(grad_kernel, int(last), negs),
        grid=(blocks,),
        in_specs=[SCALARS] + [smem_block(BLOCK)] * 2 + [PAIRS] * 3 + [WIDE] * 2 + [ROW] * 3 + [NEGS] * 2
        + [ANYWHERE] * len(before),
        out_specs=[ANYWHERE] * len(shapes) + [PAIRS, pl.BlockSpec(neg_pairs, flat), pl.BlockSpec((1, LANES), flat)],
        out_shape=[
            jax.ShapeDtypeStruct(shape, jnp.float32)
            for shape in shapes + [(2 * blocks * BLOCK, LANES), neg_pairs, (1, LANES)]
        ],
        scratch_shapes=[
            pltpu.VMEM(ent_shape, jnp.float32),
            pltpu.VMEM(rel_shape, jnp.float32),
            pltpu.VMEM((2 * BLOCK, LANES), jnp.float32),
            pltpu.VMEM((2 * BLOCK, LANES), jnp.float32),
            pltpu.VMEM((2 * LANES, 2 * LANES), jnp.float32),
            pltpu.SemaphoreType.DMA((3,)),
        ],
        compiler_params=pltpu.CompilerParams(**PARAMS),
        cost_estimate=pl.CostEstimate(flops=300_000_000, bytes_accessed=200_000_000, transcendentals=2_000_000),
        name="bucket_grads",
    )(core, *ids, *rows, *queries, *scores, weight, *negatives, *before)


def add_kernel(negs, tail_ref, neg_ref, rows_ref, n_ref, base_hbm, g_hbm, *rest):
    sum_refs, (acc, sem) = rest[:-2], rest[-2:]
    block = pl.program_id(0)

    @pl.when(block == 0)
    def _():
        copy = pltpu.make_async_copy(base_hbm, acc, sem)
        copy.start()
        copy.wait()
        small = 8

        def more(step, carry):
            for sub in range(small):
                row = step * small + sub
                at = pair_at(neg_ref[0, 0, row])
                acc[at, :] = acc[at, :] + n_ref[pair_at(2 * row), :]
            return carry

        lax.fori_loop(0, negs // small, more, 0)

    unroll = 16

    def some(step, carry):
        for sub in range(unroll):
            edge = step * unroll + sub
            at = pair_at(tail_ref[0, 0, edge])
            acc[at, :] = acc[at, :] + rows_ref[pair_at(2 * edge), :]
        return carry

    lax.fori_loop(0, BLOCK // unroll, some, 0)

    @pl.when(block == pl.num_programs(0) - 1)
    def _():
        copy = pltpu.make_async_copy(acc, g_hbm, sem)
        copy.start()
        for sum_ref in sum_refs:
            width = sum_ref.shape[-1]

            def square(step, carry):
                start = pl.multiple_of(step * 2 * width, 2 * width)
                real = acc[pl.ds(start, width, stride=2), :]
                imag = acc[pl.ds(start + 1, width, stride=2), :]
                sum_ref[step] = jnp.sum((real * real + imag * imag).T, axis=0, keepdims=True)
                return carry

            lax.fori_loop(0, sum_ref.shape[0], square, 0)
        copy.wait()


def add_rows(base, tail_ids, neg_ids, rows, neg_rows, sum_shape):
    blocks = tail_ids.shape[0]
    sums = [] if sum_shape is None else [sum_shape]
    return pl.pallas_call(
        functools.partial(add_kernel, neg_ids.shape[-1]),
        grid=(blocks,),
        in_specs=[smem_block(BLOCK), SCALARS, PAIRS, pl.BlockSpec(neg_rows.shape, lambda b: (0, 0)), ANYWHERE],
        out_specs=[ANYWHERE] + [pl.BlockSpec(shape, lambda b: (0, 0, 0)) for shape in sums],
        out_shape=[jax.ShapeDtypeStruct(shape, jnp.float32) for shape in [base.shape] + sums],
        scratch_shapes=[pltpu.VMEM(base.shape, jnp.float32), pltpu.SemaphoreType.DMA],
        compiler_params=pltpu.CompilerParams(**PARAMS),
        cost_estimate=pl.CostEstimate(flops=100_000_000, bytes_accessed=100_000_000, transcendentals=0),
        name="add_rows",
    )(tail_ids, neg_ids, rows, neg_rows, base)


def square_kernel(one_ref, two_ref, *rest):
    g_ref, sum_ref = rest[-2:]
    g_ref[...] = one_ref[...] + two_ref[...]
    real, imag = halves(g_ref)
    sum_ref[0] = jnp.sum((real * real + imag * imag).T, axis=0, keepdims=True)


def step_kernel(rate, dim, par_ref, g_ref, state_ref, sm_ref, sp_ref, out_ref, new_ref, *bf_refs):
    state = state_ref[0] + (sm_ref[0] + sp_ref[0]) / dim
    new_ref[0] = state
    scale = column(rate / jnp.sqrt(state + ADA_EPS))
    p_re, p_im = halves(par_ref)
    g_re, g_im = halves(g_ref)
    put_halves(out_ref, p_re - g_re * scale, p_im - g_im * scale)
    for ref in bf_refs:
        ref[...] = out_ref[...].astype(jnp.bfloat16)


PAIR_ROWS = pl.BlockSpec((2 * WIDE_ROWS, LANES), lambda b: (b, 0))
WIDE_ROW = pl.BlockSpec((1, 1, WIDE_ROWS), lambda b: (b, 0, 0))


def square_sums(one, two, blocks, after):
    return pl.pallas_call(
        square_kernel,
        grid=(blocks,),
        in_specs=[PAIR_ROWS, PAIR_ROWS] + [ANYWHERE] * len(after),
        out_specs=[PAIR_ROWS, WIDE_ROW],
        out_shape=[
            jax.ShapeDtypeStruct(one.shape, jnp.float32),
            jax.ShapeDtypeStruct((blocks, 1, WIDE_ROWS), jnp.float32),
        ],
        compiler_params=pltpu.CompilerParams(dimension_semantics=("arbitrary",)),
        cost_estimate=pl.CostEstimate(flops=4 * one.size, bytes_accessed=12 * one.size, transcendentals=0),
        name="square_sums",
    )(one, two, *after)


def adagrad_step(param, state, grad, sums, rate, dim, swap, with_bf):
    sums_peer = lax.ppermute(sums, "data", swap)
    kinds = [jnp.float32, jnp.bfloat16] if with_bf else [jnp.float32]
    wide = [jax.ShapeDtypeStruct(param.shape, kind) for kind in kinds]
    return pl.pallas_call(
        functools.partial(step_kernel, rate, dim),
        grid=(state.shape[0],),
        in_specs=[PAIR_ROWS, PAIR_ROWS, WIDE_ROW, WIDE_ROW, WIDE_ROW],
        out_specs=[PAIR_ROWS, WIDE_ROW] + [PAIR_ROWS] * (len(kinds) - 1),
        out_shape=[wide[0], jax.ShapeDtypeStruct(state.shape, jnp.float32)] + wide[1:],
        compiler_params=pltpu.CompilerParams(dimension_semantics=("arbitrary",)),
        cost_estimate=pl.CostEstimate(flops=4 * param.size, bytes_accessed=12 * param.size, transcendentals=0),
        name="adagrad_step",
    )(param, grad, state, sums, sums_peer)


def join_kernel(part_ref, mine_ref, peer_ref, *rest):
    out_ref = rest[-1]
    second = part_ref[0] != 0
    width = mine_ref.shape[0] // 2
    for side in range(2):
        mine, peer = (ref[pl.ds(side * width, width), :] for ref in (mine_ref, peer_ref))
        out_ref[pl.ds(2 * side * width, width), :] = jnp.where(second, peer, mine)
        out_ref[pl.ds((2 * side + 1) * width, width), :] = jnp.where(second, mine, peer)


def join_columns(part, mine, peer, start=0, total=None, whole=()):
    width, rows = mine.shape
    skip = start // WIDE_ROWS
    half = pl.BlockSpec((width, WIDE_ROWS), lambda b: (0, b))
    return pl.pallas_call(
        join_kernel,
        grid=(pl.cdiv(rows, WIDE_ROWS),),
        in_specs=[SCALARS, half, half] + [ANYWHERE] * len(whole),
        out_specs=pl.BlockSpec((2 * width, WIDE_ROWS), lambda b: (0, b + skip)),
        out_shape=jax.ShapeDtypeStruct((2 * width, total or rows), jnp.float32),
        input_output_aliases={3: 0} if whole else {},
        compiler_params=pltpu.CompilerParams(dimension_semantics=("arbitrary",)),
        cost_estimate=pl.CostEstimate(flops=mine.size, bytes_accessed=16 * mine.size, transcendentals=0),
        name="join_columns",
    )(part[None], mine, peer, *whole)


def solution(mesh):
    ent_size = mesh.shape["ent"]
    data_size = mesh.shape["data"]
    swap = [(src, data_size - 1 - src) for src in range(data_size)]
    core_swap = [(src, src ^ 1) for src in range(ent_size)]
    chip_swap = [(src, src ^ 2) for src in range(ent_size)]

    def device_epoch(ent_table, ada_state, rel_table, head_idx, tail_idx, rel_idx, edge_mask, neg_idx):
        ent_rows, dim = ent_table.shape
        rel_rows = rel_table.shape[0]
        edge_count = head_idx.shape[-1]
        negs = neg_idx.shape[-1]
        part = lax.axis_index("data")
        core = lax.rem(lax.axis_index("ent"), 2)
        core_at = core[None]
        ent, table = split_columns(ent_table, part, True)
        rel = split_columns(rel_table, part, False)[0]
        ent_shape, rel_shape = ent.shape, rel.shape
        rel_mine = lax.dynamic_slice_in_dim(rel, core * rel_rows, rel_rows, axis=0)
        rel_other = lax.dynamic_slice_in_dim(rel, (1 - core) * rel_rows, rel_rows, axis=0)
        state = ada_state.reshape(-1, 1, WIDE_ROWS)
        rel_state = jnp.zeros((pl.cdiv(rel_rows // 2, WIDE_ROWS), 1, WIDE_ROWS), jnp.float32)

        local = jnp.concatenate(
            [2 * head_idx[0, 0], 2 * tail_idx[0, 0], 2 * rel_idx[0, 0], edge_mask[0, 0], 2 * neg_idx[0, 0]], axis=1)
        both = lax.all_gather(local, "data")
        blocks = edge_count // BLOCK

        def field(slot, bucket, round_idx):
            return both[bucket, round_idx, slot * edge_count:(slot + 1) * edge_count].reshape(blocks, 1, BLOCK)

        def owned(round_idx):
            mine = jnp.concatenate(
                [both[:, round_idx, edge_count:2 * edge_count], both[:, round_idx, 4 * edge_count:]], axis=1)
            if round_idx:
                mine = lax.ppermute(mine, "ent", [(src, (src + round_idx) % ent_size) for src in range(ent_size)])
            return [
                (mine[bucket, :edge_count].reshape(blocks, 1, BLOCK), mine[bucket, edge_count:].reshape(1, 1, negs))
                for bucket in range(data_size)
            ]

        losses = []
        for round_idx in range(ent_size):
            if round_idx:
                fetch = [((dest + round_idx) % ent_size, dest) for dest in range(ent_size)]
                table = lax.ppermute(table, "ent", fetch)
            ids = [[field(slot, bucket, round_idx) for slot in range(3)] for bucket in range(data_size)]
            asked = []
            for bucket in range(data_size):
                asked.append(query_rows(core_at, ent, rel_mine, rel_other, ids[bucket][0], ids[bucket][2]))
            back = [(src, (src + round_idx) % ent_size) for src in range(ent_size)]
            targets = owned(round_idx)
            before = None
            sums, returned = [], []
            for bucket in range(data_size):
                a_rows, r_rows, q_mine = asked[bucket]
                q_peer = lax.ppermute(q_mine, "data", swap)
                neg_ids = both[bucket, round_idx, 4 * edge_count:].reshape(1, 1, negs)
                c_rows, p_mine, m_mine = tail_rows(table, ids[bucket][1], neg_ids, a_rows, r_rows)
                m_peer = lax.ppermute(m_mine, "data", swap)
                p_peer = lax.ppermute(p_mine, "data", swap)
                *before, t_rows, n_rows, loss = bucket_grads(
                    core_at, (ids[bucket][0], ids[bucket][2]), negs, (a_rows, r_rows, c_rows), (q_mine, q_peer),
                    (p_mine, p_peer), field(3, bucket, round_idx).astype(jnp.float32), (m_mine, m_peer), before,
                    ent_shape, rel_shape)
                sums.append(loss[0, 0])
                if round_idx:
                    t_rows = lax.ppermute(t_rows, "ent", back)
                    n_rows = lax.ppermute(n_rows, "ent", back)
                returned.append((t_rows, n_rows))
            g_ent, keep, give = before
            chip_sum = keep + lax.ppermute(give, "ent", core_swap)
            chip_other = lax.ppermute(chip_sum, "ent", chip_swap)
            for bucket in range(data_size):
                shape = state.shape if bucket == data_size - 1 else None
                g_ent, *ent_sums = add_rows(g_ent, *targets[bucket], *returned[bucket], shape)
            ent, state, table = adagrad_step(ent, state, g_ent, ent_sums[0], LEARN_ENT, dim, swap, True)
            after = state
            if round_idx == ent_size - 1:
                size = ent_rows // PIECES
                ent_cols = [flip_half(ent, dim, piece * size, size) for piece in range(PIECES)]
                after = ent_cols[0]
                ent_peer = []
                for piece in range(PIECES):
                    ent_peer.append(lax.ppermute(ent_cols[piece], "data", swap))
            g_rel, rel_sums = square_sums(chip_sum, chip_other, rel_state.shape[0], (after,))
            rel_mine, rel_state = adagrad_step(rel_mine, rel_state, g_rel, rel_sums, LEARN_REL, dim, swap, False)
            if round_idx < ent_size - 1:
                rel_other = lax.ppermute(rel_mine, "ent", core_swap)
            losses.append(jnp.where(part == 0, sums[0], sums[1]) / edge_count)

        rel_cols = flip_half(rel_mine, dim)
        quarter = rel_cols.shape[-1] // 2
        chip = lax.axis_index("ent") // 2
        piece = lax.ppermute(lax.dynamic_slice_in_dim(rel_cols, chip * quarter, quarter, axis=1), "data", swap)
        piece_other = lax.ppermute(piece, "ent", chip_swap)
        rel_peer = jnp.concatenate(
            [jnp.where(chip == 0, piece, piece_other), jnp.where(chip == 0, piece_other, piece)], axis=1)
        rel_all = join_columns(part, rel_cols, rel_peer)
        rel_other = lax.ppermute(rel_all, "ent", core_swap)
        rel_out = jnp.concatenate(
            [jnp.where(core == 0, rel_all, rel_other), jnp.where(core == 0, rel_other, rel_all)], axis=1)
        ent_out = ()
        for piece in range(PIECES):
            if piece == PIECES - 1:
                ent_out = ent_out + (rel_out,)
            ent_out = (join_columns(part, ent_cols[piece], ent_peer[piece], piece * size, ent_rows, ent_out),)
        ent_out, rel_out = ent_out[0].T, rel_out.T
        return ent_out, state.reshape(-1), rel_out, jnp.stack(losses)[None, None, :]

    ent_spec = P(("sweep", "ent"), None)
    row_spec = P(("sweep", "ent"))
    rel_spec = P("sweep", None)
    edge_spec = P(("sweep", "ent"), "data", None, None)
    loss_spec = P(("sweep", "ent"), "data", None)
    return jax.shard_map(
        device_epoch, mesh=mesh,
        in_specs=(ent_spec, row_spec, rel_spec, edge_spec, edge_spec, edge_spec, edge_spec, edge_spec),
        out_specs=(ent_spec, row_spec, rel_spec, loss_spec),
        check_vma=False)
```
